16 devices in a mesh: dp: 4 (over y, z, core), tp: 4 (over x).
Axes of the slice: x: 4, y: 2, z: 1, core: 2. Of those that a mesh axis runs over, the one named last changes fastest.
The devices are a block of a 4x4x8 slice.
Arguments:
- x: bfloat16 [4096, 4096], P(('dp', 'tp')), parts along dimension 0
- gain: bfloat16 [4096], replicated
- wq: bfloat16 [4096, 8192], P(None, 'tp')
- wk: bfloat16 [4096, 512], P(None, 'tp')
- wv: bfloat16 [4096, 512], P(None, 'tp')
- wo: bfloat16 [8192, 4096], P('tp')
Outputs:
- output: bfloat16 [4096, 4096], P(('dp', 'tp')), parts along dimension 0
There are 4 independent parts. The reference program is written for one: setup_inputs(seed, part) draws one part's arguments, and reference() takes and returns one part's arrays. A program takes and returns all parts, laid end to end along the dimension named above; an argument that names none is the same for every part.
All inputs are finite; a program needn't handle non-finite values.
Results may differ from the reference program's by a relative error of at most 0.012.
Values are sent between devices in bfloat16 or wider.
A program may use at most 768 MiB of HBM per device.

```python
import jax
import jax.numpy as jnp
from jax import lax

ROWS = 1024
D = 4096
HEADS = 64
KV_HEADS = 4
HEAD = 128
THETA = 10000


def setup_inputs(seed: int = 0, part: int = 0) -> dict:
    kx, kn, kq, kk, kv, ko = jax.random.split(jax.random.key(seed), 6)

    def weights(key, rows, columns):
        return jax.random.normal(key, (rows, columns), jnp.float32) * rows**-0.5

    drawn = {
        "x": jax.random.normal(jax.random.fold_in(kx, part), (ROWS, D), jnp.float32),
        "gain": 1 + 0.1 * jax.random.normal(kn, (D,), jnp.float32),
        "wq": 2 * weights(kq, D, HEADS * HEAD),
        "wk": 2 * weights(kk, D, KV_HEADS * HEAD),
        "wv": 4 * weights(kv, D, KV_HEADS * HEAD),
        "wo": weights(ko, HEADS * HEAD, D),
    }
    return {k: v.astype(jnp.bfloat16) for k, v in drawn.items()}


def normed(x, gain):
    wide = x.astype(jnp.float32)
    scale = lax.rsqrt(jnp.mean(wide * wide, -1, keepdims=True) + 1e-6)
    return (wide * scale * gain.astype(jnp.float32)).astype(jnp.bfloat16)


def turned(t, place, theta):
    half = t.shape[-1] // 2
    angle = place.astype(jnp.float32)[:, None] * theta ** (-jnp.arange(half, dtype=jnp.float32) / half)
    cos, sin = jnp.cos(angle)[:, None], jnp.sin(angle)[:, None]
    a, b = t[..., :half].astype(jnp.float32), t[..., half:].astype(jnp.float32)
    return jnp.concatenate([a * cos - b * sin, b * cos + a * sin], -1).astype(jnp.bfloat16)


def matmul(a, w):
    return jnp.dot(a, w, preferred_element_type=jnp.float32).astype(jnp.bfloat16)


def einsum(form, a, b):
    return jnp.einsum(form, a.astype(jnp.float32), b.astype(jnp.float32))


def attention(q, k, v):
    scores = einsum("tgsd,ugd->gstu", q, k) * q.shape[-1] ** -0.5
    token = jnp.arange(q.shape[0])
    scores = jnp.where(token[:, None] >= token, scores, -jnp.inf)
    weights = jax.nn.softmax(scores, -1).astype(jnp.bfloat16)
    return einsum("gstu,ugd->tgsd", weights, v).astype(jnp.bfloat16)


def reference(x, gain, wq, wk, wv, wo):
    a, place = normed(x, gain), jnp.arange(ROWS)
    q = turned(matmul(a, wq).reshape(ROWS, HEADS, HEAD), place, THETA).reshape(ROWS, KV_HEADS, -1, HEAD)
    k = turned(matmul(a, wk).reshape(ROWS, KV_HEADS, HEAD), place, THETA)
    v = matmul(a, wv).reshape(ROWS, KV_HEADS, HEAD)
    seen = attention(q, k, v).reshape(ROWS, HEADS * HEAD)
    return (x.astype(jnp.float32) + jnp.dot(seen, wo, preferred_element_type=jnp.float32)).astype(jnp.bfloat16)
```

```python
import functools

import jax
import jax.numpy as jnp
import numpy as np
from jax import lax
from jax.experimental import pallas as pl
from jax.experimental.pallas import tpu as pltpu
from jax.sharding import PartitionSpec as P

HEAD = 128
THETA = 10000
NEG = -1e30
HIDDEN = 2 * NEG
LOG2E = 1.4426950408889634
SUB = 2
QT = 256
CW = 256
UNROLL = 4
EXTRA = 16


def _dot(a, b, ca=1, cb=0):
    return lax.dot_general(a, b, (((ca,), (cb,)), ((), ())), preferred_element_type=jnp.float32)


def _kernel(n, x_ref, gain_ref, wq_ref, wk_ref, wv_ref, wo_ref, tab_ref, y_ref,
            xs, gs, xg, wq, wkv, tab, q, k, vt, mix, top, wob, sbuf, rbuf,
            x_sem, g_sem, wq_sem, w_sem, wo_sem, ag_send, ag_recv, rs_send, rs_recv, out_sem):
    rows, width = x_ref.shape
    half = rows // 2
    sub = half // SUB
    qwidth = wq_ref.shape[1]
    heads = qwidth // HEAD
    hw = width // 2
    nc = hw // CW
    qn = qwidth // QT
    bf16, f32 = jnp.bfloat16, jnp.float32

    me = lax.axis_index("tp")
    right, left, opp = lax.rem(me + 1, n), lax.rem(me + n - 1, n), lax.rem(me + 2, n)

    def x_copy(i):
        at = pl.ds(i * sub, sub)
        return pltpu.make_async_copy(x_ref.at[at], xs.at[at], x_sem.at[i])

    def wq_copy(i):
        at = pl.ds(pl.multiple_of(i * QT, QT), QT)
        return pltpu.make_async_copy(wq_ref.at[:, at], wq.at[:, at], wq_sem.at[i])

    def wo_copy(step, s):
        c = lax.rem(step, nc)
        slot = lax.rem(step, 2)
        return pltpu.make_async_copy(wo_ref.at[:, pl.ds(pl.multiple_of(s * hw + c * CW, CW), CW)], wob.at[slot, s], wo_sem.at[slot, s])

    g_copy = pltpu.make_async_copy(gain_ref, gs, g_sem)
    tab_copy = pltpu.make_async_copy(tab_ref, tab, w_sem.at[2])
    wk_copy = pltpu.make_async_copy(wk_ref, wkv.at[:, pl.ds(0, HEAD)], w_sem.at[0])
    wv_copy = pltpu.make_async_copy(wv_ref, wkv.at[:, pl.ds(HEAD, HEAD)], w_sem.at[1])

    order = [p * SUB + i for i in range(SUB) for p in range(2)]
    g_copy.start()
    for i in order:
        x_copy(i).start()
    wk_copy.start()
    wv_copy.start()
    tab_copy.start()
    for i in range(qn):
        wq_copy(i).start()
    for s in range(2):
        wo_copy(0, s).start()

    barrier = pltpu.get_barrier_semaphore()
    for neighbour in (left, right):
        pl.semaphore_signal(barrier, inc=1, device_id={"tp": neighbour}, device_id_type=pl.DeviceIdType.MESH)
    pl.semaphore_wait(barrier, 2)

    SRC = ((0, half, 2 * half), (half, 0, 3 * half))
    DST = ((2 * half, 4 * half, 6 * half), (3 * half, 5 * half, 7 * half))

    def ag(way, leg, i):
        return pltpu.make_async_remote_copy(
            src_ref=xg.at[pl.ds(SRC[way][leg] + i * sub, sub)],
            dst_ref=xg.at[pl.ds(DST[way][leg] + i * sub, sub)],
            send_sem=ag_send.at[way, leg, i],
            recv_sem=ag_recv.at[way, leg, i],
            device_id={"tp": (right, left)[way]},
            device_id_type=pl.DeviceIdType.MESH,
        )

    g_copy.wait()
    step16 = 16

    def norm(start, count):
        def body(t, _):
            at = pl.ds(pl.multiple_of(start + t * step16, step16), step16)
            wide = xs[at, :].astype(f32)
            scale = lax.rsqrt(jnp.mean(wide * wide, -1, keepdims=True) + 1e-6)
            xg[at, :] = (wide * scale * gs[...].astype(f32)).astype(bf16)

        lax.fori_loop(0, count // step16, body, None)

    for i in range(SUB):
        for p in range(2):
            x_copy(p * SUB + i).wait()
            norm(p * half + i * sub, sub)
            ag(p, 0, i).start()
    for i in range(SUB):
        for p in range(2):
            ag(p, 1, i).start()

    lane = lax.broadcasted_iota(jnp.int32, (1, HEAD), 1)
    low = lane < HEAD // 2

    def turn(t, at):
        cs = tab[pl.ds(pl.multiple_of(at, half), half), :]
        sc = pltpu.roll(cs, HEAD // 2, 1)
        t = t.astype(f32)
        return (t * jnp.where(low, cs, sc) + pltpu.roll(t, HEAD // 2, 1) * jnp.where(low, -sc, cs)).astype(bf16)

    A, B = 0, half
    GROUPS = (((me, 0), (me, 1)), ((left, 0), (right, 1)), ((left, 1), (right, 0)), ((opp, 0), (opp, 1)))

    def project_kv(g):
        t = _dot(xg[pl.ds(g * rows, rows), :], wkv[...]).astype(bf16)
        for p, (b, h) in enumerate(GROUPS[g]):
            part = t[p * half : (p + 1) * half]
            at = pl.multiple_of(b * rows + h * half, half)
            k[pl.ds(at, half), :] = turn(part[:, :HEAD], at)
            vt[b, :HEAD, h * half : (h + 1) * half] = part[:, HEAD:].astype(f32).T.astype(bf16)

    def project_q(g):
        def body(j, _):
            if g == 0:
                wq_copy(j).wait()
            t = _dot(xg[pl.ds(g * rows, rows), :], wq[:, pl.ds(pl.multiple_of(j * QT, QT), QT)]).astype(bf16)
            for p, (b, h) in enumerate(GROUPS[g]):
                at = pl.multiple_of(b * rows + h * half, half)
                for e in range(QT // HEAD):
                    part = t[p * half : (p + 1) * half, e * HEAD : (e + 1) * HEAD]
                    q[pl.ds(at, half), pl.ds(pl.multiple_of(j * QT + e * HEAD, HEAD), HEAD)] = turn(part, at)

        lax.fori_loop(0, qn, body, None)

    e2 = HEAD**-0.5 * LOG2E

    def pair(i, j, masked):
        kj = k[pl.ds(pl.multiple_of(j * rows, rows), rows), :]
        vj = vt[j]
        if masked:
            ok = lax.broadcasted_iota(jnp.int32, (rows, rows), 0) <= lax.broadcasted_iota(jnp.int32, (rows, rows), 1)

        def body(m, _):
            hs = [m * UNROLL + u for u in range(UNROLL)]
            scores = [_dot(kj, q[pl.ds(pl.multiple_of(i * rows, rows), rows), pl.ds(pl.multiple_of(h * HEAD, HEAD), HEAD)], 1, 1) for h in hs]
            weights, keeps = [], []
            for h, s in zip(hs, scores):
                if masked:
                    s = jnp.where(ok, s, HIDDEN)
                old = top[i, h, 0:1, :]
                new = jnp.maximum(old, s.max(axis=0, keepdims=True))
                top[i, h, 0:1, :] = new
                weights.append(jnp.exp2((s - new) * e2).astype(bf16))
                keeps.append(jnp.exp2((old - new) * e2))
            for h, p, keep in zip(hs, weights, keeps):
                mix[i, h] = mix[i, h] * keep + _dot(vj, p)

        lax.fori_loop(0, heads // UNROLL, body, None)

    def pairs(wanted):
        def body(t, _):
            i, j = t // n, lax.rem(t, n)

            @pl.when((i > j) & wanted(i, j))
            def _():
                pair(i, j, False)

            @pl.when((i == j) & wanted(i, j))
            def _():
                pair(i, j, True)

        lax.fori_loop(0, n * n, body, None)

    def finish(i):
        def body(h, _):
            out = mix[i, h, :HEAD, :] * (1 / mix[i, h, HEAD : HEAD + 1, :])
            q[pl.ds(pl.multiple_of(i * rows, rows), rows), pl.ds(pl.multiple_of(h * HEAD, HEAD), HEAD)] = out.T.astype(bf16)

        lax.fori_loop(0, heads, body, None)

    tab_copy.wait()
    wk_copy.wait()
    wv_copy.wait()
    project_kv(0)
    project_q(0)

    def clear(t, _):
        i, h = t // heads, lax.rem(t, heads)
        mix[i, h] = jnp.zeros((HEAD + EXTRA, rows), f32)
        top[i, h] = jnp.full((8, rows), NEG, f32)

    lax.fori_loop(0, n * heads, clear, None)
    for b in range(n):
        vt[b, HEAD:, :] = jnp.ones((EXTRA, rows), bf16)
    pair(me, me, True)

    for i in range(SUB):
        for way in range(2):
            ag(way, 0, i).wait_recv()
            ag(way, 2, i).start()
    project_kv(1)
    project_q(1)
    for i in range(SUB):
        for way in range(2):
            ag(way, 1, i).wait_recv()
    project_kv(2)
    project_q(2)
    pairs(lambda i, j: (i != opp) & (j != opp) & ((i != me) | (j != me)))

    for i in range(SUB):
        for way in range(2):
            ag(way, 2, i).wait_recv()
    project_kv(3)
    pairs(lambda i, j: (j == opp) & (i != opp) & (i != me))
    finish(right)
    finish(left)

    def rs(way, leg, c):
        return pltpu.make_async_remote_copy(
            src_ref=sbuf.at[way, leg * nc + c],
            dst_ref=rbuf.at[way, leg * nc + c],
            send_sem=rs_send.at[way, leg * nc + c],
            recv_sem=rs_recv.at[way, leg * nc + c],
            device_id={"tp": (right, left)[way]},
            device_id_type=pl.DeviceIdType.MESH,
        )

    def attended(b):
        return q[pl.ds(pl.multiple_of(b * rows, rows), rows), :]

    def tiles(leg, c):
        step = leg * nc + c

        @pl.when(step + 1 < 4 * nc)
        def _():
            for s in range(2):
                wo_copy(step + 1, s).start()

        for s in range(2):
            wo_copy(step, s).wait()
        return lax.rem(step, 2)

    def leg0(c, _):
        slot = tiles(0, c)
        sbuf[0, c] = _dot(attended(right), wob[slot, 1]).astype(bf16)
        rs(0, 0, c).start()
        sbuf[1, c] = _dot(attended(left), wob[slot, 0]).astype(bf16)
        rs(1, 0, c).start()

    def leg1(c, _):
        slot = tiles(1, c)
        for way in range(2):
            sbuf[way, nc + c] = _dot(attended(opp), wob[slot, way]).astype(bf16)
            rs(way, 1, c).start()

    def leg2(c, _):
        slot = tiles(2, c)
        for way, b in enumerate((right, left)):
            term = _dot(attended(b), wob[slot, way])
            rs(way, 1, c).wait_recv()
            sbuf[way, 2 * nc + c] = (term + rbuf[way, nc + c].astype(f32)).astype(bf16)
            rs(way, 2, c).start()

    def y_copy(s, c):
        at = pl.ds(pl.multiple_of(s * hw + c * CW, CW), CW)
        return pltpu.make_async_copy(xs.at[:, at], y_ref.at[:, at], out_sem.at[s, c])

    def leg3(c, _):
        slot = tiles(3, c)
        for s in range(2):
            at = pl.ds(pl.multiple_of(s * hw + c * CW, CW), CW)
            term = _dot(attended(me), wob[slot, s]) + xs[:, at].astype(f32)
            rs(1 - s, 0, c).wait_recv()
            term += rbuf[1 - s, c].astype(f32)
            rs(s, 2, c).wait_recv()
            xs[:, at] = (term + rbuf[s, 2 * nc + c].astype(f32)).astype(bf16)
            y_copy(s, c).start()

    lax.fori_loop(0, nc, leg0, None)
    project_q(3)
    pairs(lambda i, j: (i == opp) | ((j == opp) & (i == me)))
    finish(opp)
    lax.fori_loop(0, nc, leg1, None)
    finish(me)
    lax.fori_loop(0, nc, leg2, None)
    lax.fori_loop(0, nc, leg3, None)

    for way in range(2):
        for leg in range(3):
            for i in range(SUB):
                ag(way, leg, i).wait_send()

    def drain(c, _):
        for way in range(2):
            for leg in range(3):
                rs(way, leg, c).wait_send()
        for s in range(2):
            y_copy(s, c).wait()

    lax.fori_loop(0, nc, drain, None)


def _table(tokens):
    half = HEAD // 2
    angle = np.arange(tokens, dtype=np.float64)[:, None] * float(THETA) ** (-np.arange(half, dtype=np.float64) / half)
    return np.concatenate([np.cos(angle), np.sin(angle)], -1).astype(np.float32)


def solution(mesh):
    n = mesh.shape["tp"]

    def step(x, gain, wq, wk, wv, wo):
        rows, width = x.shape
        tokens, qwidth = n * rows, wq.shape[1]
        heads = qwidth // HEAD
        nc = width // 2 // CW
        bf16, f32 = jnp.bfloat16, jnp.float32
        dma = pltpu.SemaphoreType.DMA
        hbm = pl.BlockSpec(memory_space=pl.ANY)
        return pl.pallas_call(
            functools.partial(_kernel, n),
            out_shape=jax.ShapeDtypeStruct((rows, width), bf16),
            in_specs=[hbm] * 7,
            out_specs=hbm,
            scratch_shapes=[
                pltpu.VMEM((rows, width), bf16),
                pltpu.VMEM((1, width), bf16),
                pltpu.VMEM((tokens, width), bf16),
                pltpu.VMEM((width, qwidth), bf16),
                pltpu.VMEM((width, 2 * HEAD), bf16),
                pltpu.VMEM((tokens, HEAD), f32),
                pltpu.VMEM((tokens, qwidth), bf16),
                pltpu.VMEM((tokens, HEAD), bf16),
                pltpu.VMEM((n, HEAD + EXTRA, rows), bf16),
                pltpu.VMEM((n, heads, HEAD + EXTRA, rows), f32),
                pltpu.VMEM((n, heads, 8, rows), f32),
                pltpu.VMEM((2, 2, qwidth, CW), bf16),
                pltpu.VMEM((2, 3 * nc, rows, CW), bf16),
                pltpu.VMEM((2, 3 * nc, rows, CW), bf16),
                dma((2 * SUB,)), dma, dma((qwidth // QT,)), dma((3,)), dma((2, 2)),
                dma((2, 3, SUB)), dma((2, 3, SUB)), dma((2, 3 * nc)), dma((2, 3 * nc)), dma((2, nc)),
            ],
            compiler_params=pltpu.CompilerParams(collective_id=0, has_side_effects=True, vmem_limit_bytes=67043328),
        )(x, gain.reshape(1, width), wq, wk, wv, wo, _table(tokens))

    tokens, columns = P(("dp", "tp"), None), P(None, "tp")
    return jax.shard_map(
        step,
        mesh=mesh,
        in_specs=(tokens, P(None), columns, columns, columns, P("tp", None)),
        out_specs=tokens,
        check_vma=False,
    )
```

```python
import functools

import jax
import jax.numpy as jnp
import numpy as np
from jax import lax
from jax.experimental import pallas as pl
from jax.experimental.pallas import tpu as pltpu
from jax.sharding import PartitionSpec as P

HEAD = 128
THETA = 10000
NEG = -1e30
HIDDEN = 2 * NEG
LOG2E = 1.4426950408889634
SUB = 2
QT = 256
CW = 256
UNROLL = 8
DEPTH = 3
EXTRA = 16


def _dot(a, b, ca=1, cb=0):
    return lax.dot_general(a, b, (((ca,), (cb,)), ((), ())), preferred_element_type=jnp.float32)


def _kernel(n, x_ref, gain_ref, wq_ref, wk_ref, wv_ref, wo_ref, tab_ref, y_ref,
            xs, gs, xg, wq, wkv, tab, q, k, vt, mix, top, wob, sbuf, rbuf,
            x_sem, g_sem, wq_sem, w_sem, wo_sem, ag_send, ag_recv, rs_send, rs_recv, out_sem):
    rows, width = x_ref.shape
    half = rows // 2
    sub = half // SUB
    qwidth = wq_ref.shape[1]
    heads = qwidth // HEAD
    hw = width // 2
    nc = hw // CW
    qn = qwidth // QT
    bf16, f32 = jnp.bfloat16, jnp.float32

    me = lax.axis_index("tp")
    right, left, opp = lax.rem(me + 1, n), lax.rem(me + n - 1, n), lax.rem(me + 2, n)

    def x_copy(i):
        at = pl.ds(i * sub, sub)
        return pltpu.make_async_copy(x_ref.at[at], xs.at[at], x_sem.at[i])

    def wq_copy(i):
        at = pl.ds(pl.multiple_of(i * QT, QT), QT)
        return pltpu.make_async_copy(wq_ref.at[:, at], wq.at[:, at], wq_sem.at[i])

    def wo_copy(step, s):
        c = lax.rem(step, nc)
        slot = lax.rem(step, DEPTH)
        return pltpu.make_async_copy(wo_ref.at[:, pl.ds(pl.multiple_of(s * hw + c * CW, CW), CW)], wob.at[slot, s], wo_sem.at[slot, s])

    g_copy = pltpu.make_async_copy(gain_ref, gs, g_sem)
    tab_copy = pltpu.make_async_copy(tab_ref, tab, w_sem.at[2])
    wk_copy = pltpu.make_async_copy(wk_ref, wkv.at[:, pl.ds(0, HEAD)], w_sem.at[0])
    wv_copy = pltpu.make_async_copy(wv_ref, wkv.at[:, pl.ds(HEAD, HEAD)], w_sem.at[1])

    order = [p * SUB + i for i in range(SUB) for p in range(2)]
    barrier = pltpu.get_barrier_semaphore()
    for neighbour in (left, right):
        pl.semaphore_signal(barrier, inc=1, device_id={"tp": neighbour}, device_id_type=pl.DeviceIdType.MESH)
    g_copy.start()
    for i in order:
        x_copy(i).start()

    SRC = ((0, half, 2 * half), (half, 0, 3 * half))
    DST = ((2 * half, 4 * half, 6 * half), (3 * half, 5 * half, 7 * half))

    def ag(way, leg, i):
        return pltpu.make_async_remote_copy(
            src_ref=xg.at[pl.ds(SRC[way][leg] + i * sub, sub)],
            dst_ref=xg.at[pl.ds(DST[way][leg] + i * sub, sub)],
            send_sem=ag_send.at[way, leg, i],
            recv_sem=ag_recv.at[way, leg, i],
            device_id={"tp": (right, left)[way]},
            device_id_type=pl.DeviceIdType.MESH,
        )

    step16 = 16

    def norm(start, count):
        def body(t, _):
            at = pl.ds(pl.multiple_of(start + t * step16, step16), step16)
            wide = xs[at, :].astype(f32)
            scale = lax.rsqrt(jnp.mean(wide * wide, -1, keepdims=True) + 1e-6)
            xg[at, :] = (wide * scale * gs[...].astype(f32)[None, :]).astype(bf16)

        lax.fori_loop(0, count // step16, body, None)

    with jax.named_scope("norm"):
        g_copy.wait()
        for i in range(SUB):
            for p in range(2):
                x_copy(p * SUB + i).wait()
                if i == SUB - 1 and p == 1:
                    wk_copy.start()
                    wv_copy.start()
                    tab_copy.start()
                    for j in range(qn):
                        wq_copy(j).start()
                norm(p * half + i * sub, sub)
                if i == 0 and p == 0:
                    pl.semaphore_wait(barrier, 2)
                ag(p, 0, i).start()
        for i in range(SUB):
            for p in range(2):
                ag(p, 1, i).start()
        for ahead in range(DEPTH - 1):
            for s in range(2):
                wo_copy(ahead, s).start()

    lane = lax.broadcasted_iota(jnp.int32, (1, HEAD), 1)
    low = lane < HEAD // 2

    def turn(t, at):
        cs = tab[pl.ds(pl.multiple_of(at, half), half), :]
        sc = pltpu.roll(cs, HEAD // 2, 1)
        t = t.astype(f32)
        return (t * jnp.where(low, cs, sc) + pltpu.roll(t, HEAD // 2, 1) * jnp.where(low, -sc, cs)).astype(bf16)

    A, B = 0, half
    GROUPS = (((me, 0), (me, 1)), ((left, 0), (right, 1)), ((left, 1), (right, 0)), ((opp, 0), (opp, 1)))

    def project_kv(g):
        t = _dot(xg[pl.ds(g * rows, rows), :], wkv[...]).astype(bf16)
        for p, (b, h) in enumerate(GROUPS[g]):
            part = t[p * half : (p + 1) * half]
            at = pl.multiple_of(b * rows + h * half, half)
            k[pl.ds(at, half), :] = turn(part[:, :HEAD], at)
            vt[b, :HEAD, h * half : (h + 1) * half] = part[:, HEAD:].astype(f32).T.astype(bf16)

    def project_q(g):
        def body(j, _):
            if g == 0:
                wq_copy(j).wait()
            t = _dot(xg[pl.ds(g * rows, rows), :], wq[:, pl.ds(pl.multiple_of(j * QT, QT), QT)]).astype(bf16)
            for p, (b, h) in enumerate(GROUPS[g]):
                at = pl.multiple_of(b * rows + h * half, half)
                for e in range(QT // HEAD):
                    part = t[p * half : (p + 1) * half, e * HEAD : (e + 1) * HEAD]
                    q[pl.ds(at, half), pl.ds(pl.multiple_of(j * QT + e * HEAD, HEAD), HEAD)] = turn(part, at)

        lax.fori_loop(0, qn, body, None)

    e2 = HEAD**-0.5 * LOG2E

    def pair(i, j, masked):
        kj = k[pl.ds(pl.multiple_of(j * rows, rows), rows), :]
        vj = vt[j]
        if masked:
            ok = lax.broadcasted_iota(jnp.int32, (rows, rows), 0) <= lax.broadcasted_iota(jnp.int32, (rows, rows), 1)

        def body(m, _):
            hs = [m * UNROLL + u for u in range(UNROLL)]
            scores = [_dot(kj, q[pl.ds(pl.multiple_of(i * rows, rows), rows), pl.ds(pl.multiple_of(h * HEAD, HEAD), HEAD)], 1, 1) for h in hs]
            weights, keeps = [], []
            for h, s in zip(hs, scores):
                if masked:
                    s = jnp.where(ok, s, HIDDEN)
                old = top[i, h, 0:1, :]
                new = jnp.maximum(old, s.max(axis=0, keepdims=True))
                top[i, h, 0:1, :] = new
                weights.append(jnp.exp2((s - new) * e2).astype(bf16))
                keeps.append(jnp.exp2((old - new) * e2))
            for h, p, keep in zip(hs, weights, keeps):
                mix[i, h] = mix[i, h] * keep + _dot(vj, p)

        lax.fori_loop(0, heads // UNROLL, body, None)

    def pairs(wanted):
        def body(t, _):
            i, j = t // n, lax.rem(t, n)

            @pl.when((i > j) & wanted(i, j))
            def _():
                pair(i, j, False)

            @pl.when((i == j) & wanted(i, j))
            def _():
                pair(i, j, True)

        lax.fori_loop(0, n * n, body, None)

    def finish(i):
        def body(h, _):
            out = mix[i, h, :HEAD, :] * (1 / mix[i, h, HEAD : HEAD + 1, :])
            q[pl.ds(pl.multiple_of(i * rows, rows), rows), pl.ds(pl.multiple_of(h * HEAD, HEAD), HEAD)] = out.T.astype(bf16)

        lax.fori_loop(0, heads, body, None)

    with jax.named_scope("own_proj"):
        tab_copy.wait()
        wk_copy.wait()
        wv_copy.wait()
        project_kv(0)
        project_q(0)

    def clear(t, _):
        i, h = t // heads, lax.rem(t, heads)
        mix[i, h] = jnp.zeros((HEAD + EXTRA, rows), f32)
        top[i, h] = jnp.full((8, rows), NEG, f32)

    with jax.named_scope("own_pair"):
        lax.fori_loop(0, n * heads, clear, None)
        for b in range(n):
            vt[b, HEAD:, :] = jnp.ones((EXTRA, rows), bf16)
        pair(me, me, True)

    with jax.named_scope("wait_g1"):
        for i in range(SUB):
            for way in range(2):
                ag(way, 0, i).wait_recv()
                ag(way, 2, i).start()
    with jax.named_scope("proj_g1"):
        project_kv(1)
        project_q(1)
    with jax.named_scope("wait_g2"):
        for i in range(SUB):
            for way in range(2):
                ag(way, 1, i).wait_recv()
    with jax.named_scope("proj_g2"):
        project_kv(2)
        project_q(2)
    with jax.named_scope("pairs_early"):
        pairs(lambda i, j: (i != opp) & (j != opp) & ((i != me) | (j != me)))

    with jax.named_scope("wait_g3"):
        for i in range(SUB):
            for way in range(2):
                ag(way, 2, i).wait_recv()
    with jax.named_scope("kv_g3"):
        project_kv(3)
    with jax.named_scope("pairs_sides"):
        pairs(lambda i, j: (j == opp) & (i != opp) & (i != me))
    with jax.named_scope("finish_sides"):
        finish(right)
        finish(left)

    def rs(way, leg, c):
        return pltpu.make_async_remote_copy(
            src_ref=sbuf.at[way, leg * nc + c],
            dst_ref=rbuf.at[way, leg * nc + c],
            send_sem=rs_send.at[way, leg * nc + c],
            recv_sem=rs_recv.at[way, leg * nc + c],
            device_id={"tp": (right, left)[way]},
            device_id_type=pl.DeviceIdType.MESH,
        )

    def attended(b):
        return q[pl.ds(pl.multiple_of(b * rows, rows), rows), :]

    def tiles(leg, c):
        step = leg * nc + c

        @pl.when(step + DEPTH - 1 < 4 * nc)
        def _():
            for s in range(2):
                wo_copy(step + DEPTH - 1, s).start()

        for s in range(2):
            wo_copy(step, s).wait()
        return lax.rem(step, DEPTH)

    def leg0(c, _):
        slot = tiles(0, c)
        sbuf[0, c] = _dot(attended(right), wob[slot, 1]).astype(bf16)
        sbuf[1, c] = _dot(attended(left), wob[slot, 0]).astype(bf16)
        rs(0, 0, c).start()
        rs(1, 0, c).start()

    def leg1(c, _):
        slot = tiles(1, c)
        for way in range(2):
            sbuf[way, nc + c] = _dot(attended(opp), wob[slot, way]).astype(bf16)
        for way in range(2):
            rs(way, 1, c).start()

    def leg2(c, _):
        slot = tiles(2, c)
        for way, b in enumerate((right, left)):
            term = _dot(attended(b), wob[slot, way])
            rs(way, 1, c).wait_recv()
            sbuf[way, 2 * nc + c] = (term + rbuf[way, nc + c].astype(f32)).astype(bf16)
            rs(way, 2, c).start()

    def y_copy(s, c):
        at = pl.ds(pl.multiple_of(s * hw + c * CW, CW), CW)
        return pltpu.make_async_copy(xs.at[:, at], y_ref.at[:, at], out_sem.at[s, c])

    def leg3(c, _):
        slot = tiles(3, c)
        for s in range(2):
            at = pl.ds(pl.multiple_of(s * hw + c * CW, CW), CW)
            term = _dot(attended(me), wob[slot, s]) + xs[:, at].astype(f32)
            rs(1 - s, 0, c).wait_recv()
            term += rbuf[1 - s, c].astype(f32)
            rs(s, 2, c).wait_recv()
            xs[:, at] = (term + rbuf[s, 2 * nc + c].astype(f32)).astype(bf16)
            y_copy(s, c).start()

    with jax.named_scope("leg0"):
        lax.fori_loop(0, nc, leg0, None)
    with jax.named_scope("q_g3"):
        project_q(3)
    with jax.named_scope("pairs_opp"):
        pairs(lambda i, j: (i == opp) | ((j == opp) & (i == me)))
        finish(opp)
    with jax.named_scope("leg1"):
        lax.fori_loop(0, nc, leg1, None)
    with jax.named_scope("leg2"):
        finish(me)
        lax.fori_loop(0, nc, leg2, None)
    with jax.named_scope("leg3"):
        lax.fori_loop(0, nc, leg3, None)

    for way in range(2):
        for leg in range(3):
            for i in range(SUB):
                ag(way, leg, i).wait_send()

    def drain(c, _):
        for way in range(2):
            for leg in range(3):
                rs(way, leg, c).wait_send()
        for s in range(2):
            y_copy(s, c).wait()

    lax.fori_loop(0, nc, drain, None)


def _table(tokens):
    half = HEAD // 2
    angle = np.arange(tokens, dtype=np.float64)[:, None] * float(THETA) ** (-np.arange(half, dtype=np.float64) / half)
    return np.concatenate([np.cos(angle), np.sin(angle)], -1).astype(np.float32)


def solution(mesh):
    n = mesh.shape["tp"]

    def step(x, gain, wq, wk, wv, wo):
        rows, width = x.shape
        tokens, qwidth = n * rows, wq.shape[1]
        heads = qwidth // HEAD
        nc = width // 2 // CW
        bf16, f32 = jnp.bfloat16, jnp.float32
        dma = pltpu.SemaphoreType.DMA
        hbm = pl.BlockSpec(memory_space=pl.ANY)
        return pl.pallas_call(
            functools.partial(_kernel, n),
            out_shape=jax.ShapeDtypeStruct((rows, width), bf16),
            in_specs=[hbm] * 7,
            out_specs=hbm,
            scratch_shapes=[
                pltpu.VMEM((rows, width), bf16),
                pltpu.VMEM((width,), bf16),
                pltpu.VMEM((tokens, width), bf16),
                pltpu.VMEM((width, qwidth), bf16),
                pltpu.VMEM((width, 2 * HEAD), bf16),
                pltpu.VMEM((tokens, HEAD), f32),
                pltpu.VMEM((tokens, qwidth), bf16),
                pltpu.VMEM((tokens, HEAD), bf16),
                pltpu.VMEM((n, HEAD + EXTRA, rows), bf16),
                pltpu.VMEM((n, heads, HEAD + EXTRA, rows), f32),
                pltpu.VMEM((n, heads, 8, rows), f32),
                pltpu.VMEM((DEPTH, 2, qwidth, CW), bf16),
                pltpu.VMEM((2, 3 * nc, rows, CW), bf16),
                pltpu.VMEM((2, 3 * nc, rows, CW), bf16),
                dma((2 * SUB,)), dma, dma((qwidth // QT,)), dma((3,)), dma((DEPTH, 2)),
                dma((2, 3, SUB)), dma((2, 3, SUB)), dma((2, 3 * nc)), dma((2, 3 * nc)), dma((2, nc)),
            ],
            compiler_params=pltpu.CompilerParams(collective_id=0, has_side_effects=True, vmem_limit_bytes=67043328),
        )(x, gain, wq, wk, wv, wo, _table(tokens))

    tokens, columns = P(("dp", "tp"), None), P(None, "tp")
    return jax.shard_map(
        step,
        mesh=mesh,
        in_specs=(tokens, P(None), columns, columns, columns, P("tp", None)),
        out_specs=tokens,
        check_vma=False,
    )
```

```python
import functools

import jax
import jax.numpy as jnp
import numpy as np
from jax import lax
from jax.experimental import pallas as pl
from jax.experimental.pallas import tpu as pltpu
from jax.sharding import PartitionSpec as P

HEAD = 128
THETA = 10000
NEG = -1e30
HIDDEN = 2 * NEG
LOG2E = 1.4426950408889634
SUB = 2
QT = 256
CW = 256
FINISH = 4
UNROLL = 8
DEPTH = 3
VMEM = 61 * 2**20 + 2**19
EXTRA = 16


def _dot(a, b, ca=1, cb=0):
    return lax.dot_general(a, b, (((ca,), (cb,)), ((), ())), preferred_element_type=jnp.float32)


def _kernel(n, x_ref, gain_ref, wq_ref, wk_ref, wv_ref, wo_ref, tab_ref, y_ref,
            gs, xg, wq, wkv, tab, q, k, v, mix, top, wob, sbuf, rbuf,
            x_sem, g_sem, wq_sem, w_sem, wo_sem, ag_send, ag_recv, rs_send, rs_recv):
    rows, width = x_ref.shape
    half = rows // 2
    sub = half // SUB
    qwidth = wq_ref.shape[1]
    heads = qwidth // HEAD
    hw = width // 2
    nc = hw // CW
    qn = qwidth // QT
    bf16, f32 = jnp.bfloat16, jnp.float32

    me = lax.axis_index("tp")
    right, left, opp = lax.rem(me + 1, n), lax.rem(me + n - 1, n), lax.rem(me + 2, n)

    def x_copy(i):
        at = pl.ds(i * sub, sub)
        return pltpu.make_async_copy(x_ref.at[at], y_ref.at[at], x_sem.at[i])

    def wq_copy(i):
        at = pl.ds(pl.multiple_of(i * QT, QT), QT)
        return pltpu.make_async_copy(wq_ref.at[:, at], wq.at[:, at], wq_sem.at[i])

    def wo_copy(step, s):
        c = lax.rem(step, nc)
        slot = lax.rem(step, DEPTH)
        return pltpu.make_async_copy(wo_ref.at[:, pl.ds(pl.multiple_of(s * hw + c * CW, CW), CW)], wob.at[slot, s], wo_sem.at[slot, s])

    g_copy = pltpu.make_async_copy(gain_ref, gs, g_sem)
    tab_copy = pltpu.make_async_copy(tab_ref, tab, w_sem.at[2])
    wk_copy = pltpu.make_async_copy(wk_ref, wkv.at[:, pl.ds(0, HEAD)], w_sem.at[0])
    wv_copy = pltpu.make_async_copy(wv_ref, wkv.at[:, pl.ds(HEAD, HEAD)], w_sem.at[1])

    barrier = pltpu.get_barrier_semaphore()
    for neighbour in (left, right):
        pl.semaphore_signal(barrier, inc=1, device_id={"tp": neighbour}, device_id_type=pl.DeviceIdType.MESH)
    g_copy.start()
    for i in range(2 * SUB):
        x_copy(i).start()

    def source(way, leg, i):
        if leg < 2:
            return (2 * i + (leg if way == 0 else 1 - leg)) * sub
        return rows + way * half + i * sub

    def target(way, leg, i):
        if leg < 2:
            return (leg + 1) * rows + way * half + i * sub
        return 3 * rows + (2 * i + way) * sub

    def ag(way, leg, i):
        return pltpu.make_async_remote_copy(
            src_ref=xg.at[pl.ds(source(way, leg, i), sub)],
            dst_ref=xg.at[pl.ds(target(way, leg, i), sub)],
            send_sem=ag_send.at[way, leg, i],
            recv_sem=ag_recv.at[way, leg, i],
            device_id={"tp": (right, left)[way]},
            device_id_type=pl.DeviceIdType.MESH,
        )

    step16 = 16

    def norm(start, count):
        def body(t, _):
            at = pl.ds(pl.multiple_of(start + t * step16, step16), step16)
            wide = y_ref[at, :].astype(f32)
            scale = lax.rsqrt(jnp.mean(wide * wide, -1, keepdims=True) + 1e-6)
            xg[at, :] = (wide * scale * gs[...].astype(f32)[None, :]).astype(bf16)

        lax.fori_loop(0, count // step16, body, None)

    with jax.named_scope("norm"):
        g_copy.wait()
        for i in range(SUB):
            for p in range(2):
                x_copy(2 * i + p).wait()
                if i == SUB - 1 and p == 1:
                    wk_copy.start()
                    wv_copy.start()
                    tab_copy.start()
                    for j in range(qn):
                        wq_copy(j).start()
                norm((2 * i + p) * sub, sub)
                if i == 0 and p == 0:
                    pl.semaphore_wait(barrier, 2)
                ag(p, 0, i).start()
        for i in range(SUB):
            for p in range(2):
                ag(p, 1, i).start()
        for ahead in range(DEPTH - 1):
            for s in range(2):
                wo_copy(ahead, s).start()

    lane = lax.broadcasted_iota(jnp.int32, (1, HEAD), 1)
    low = lane < HEAD // 2

    def turn(t, at):
        cs = tab[pl.ds(pl.multiple_of(at, sub), t.shape[0]), :]
        sc = pltpu.roll(cs, HEAD // 2, 1)
        t = t.astype(f32)
        return (t * jnp.where(low, cs, sc) + pltpu.roll(t, HEAD // 2, 1) * jnp.where(low, -sc, cs)).astype(bf16)

    def runs(g):
        if g in (0, 3):
            return ((0, rows, (me if g == 0 else opp) * rows),)
        halves = ((left, 0), (right, 1)) if g == 1 else ((left, 1), (right, 0))
        return tuple((p * half + i * sub, sub, b * rows + (2 * i + h) * sub) for p, (b, h) in enumerate(halves) for i in range(SUB))

    def project_kv(g, part=None):
        first, count = (0, rows) if part is None else (part * half, half)
        t = _dot(xg[pl.ds(g * rows + first, count), :], wkv[...]).astype(bf16)
        for row, size, at in runs(g) if part is None else ((0, half, runs(g)[0][2] + first),):
            at = pl.multiple_of(at, sub)
            k[pl.ds(at, size), :] = turn(t[row : row + size, :HEAD], at)
            v[pl.ds(at, size), :] = t[row : row + size, HEAD:]

    def project_q(g):
        def body(j, _):
            if g == 0:
                wq_copy(j).wait()
            t = _dot(xg[pl.ds(g * rows, rows), :], wq[:, pl.ds(pl.multiple_of(j * QT, QT), QT)]).astype(bf16)
            for row, size, at in runs(g):
                at = pl.multiple_of(at, sub)
                for e in range(QT // HEAD):
                    part = t[row : row + size, e * HEAD : (e + 1) * HEAD]
                    q[pl.ds(at, size), pl.ds(pl.multiple_of(j * QT + e * HEAD, HEAD), HEAD)] = turn(part, at)

        lax.fori_loop(0, qn, body, None)

    e2 = HEAD**-0.5 * LOG2E

    def pair(i, j, masked, part=None):
        first, count = (0, rows) if part is None else (part * half, half)
        keys = pl.ds(pl.multiple_of(j * rows + first, half), count)
        kj = k[keys, :]
        vj = jnp.concatenate([v[keys, :].astype(f32).T.astype(bf16), jnp.ones((EXTRA, count), bf16)], axis=0)
        if masked:
            ok = lax.broadcasted_iota(jnp.int32, (rows, rows), 0) <= lax.broadcasted_iota(jnp.int32, (rows, rows), 1)

        def body(m, _):
            hs = [m * UNROLL + u for u in range(UNROLL)]
            scores = [_dot(kj, q[pl.ds(pl.multiple_of(i * rows, rows), rows), pl.ds(pl.multiple_of(h * HEAD, HEAD), HEAD)], 1, 1) for h in hs]
            weights, keeps = [], []
            for h, s in zip(hs, scores):
                if masked:
                    s = jnp.where(ok, s, HIDDEN)
                old = top[i, h, 0:1, :]
                new = jnp.maximum(old, s.max(axis=0, keepdims=True))
                top[i, h, 0:1, :] = new
                weights.append(jnp.exp2((s - new) * e2).astype(bf16))
                keeps.append(jnp.exp2((old - new) * e2))
            for h, p, keep in zip(hs, weights, keeps):
                mix[i, h] = mix[i, h] * keep + _dot(vj, p)

        lax.fori_loop(0, heads // UNROLL, body, None)

    def pairs(wanted):
        def body(t, _):
            i, j = t // n, lax.rem(t, n)

            @pl.when((i > j) & wanted(i, j))
            def _():
                pair(i, j, False)

            @pl.when((i == j) & wanted(i, j))
            def _():
                pair(i, j, True)

        lax.fori_loop(0, n * n, body, None)

    def finish(i):
        def body(m, _):
            for u in range(FINISH):
                h = m * FINISH + u
                out = mix[i, h, :HEAD, :] * (1 / mix[i, h, HEAD : HEAD + 1, :])
                q[pl.ds(pl.multiple_of(i * rows, rows), rows), pl.ds(pl.multiple_of(h * HEAD, HEAD), HEAD)] = out.T.astype(bf16)

        lax.fori_loop(0, heads // FINISH, body, None)

    with jax.named_scope("own_proj"):
        tab_copy.wait()
        wk_copy.wait()
        wv_copy.wait()
        project_kv(0)
        project_q(0)

    def clear(t, _):
        i, h = t // heads, lax.rem(t, heads)
        mix[i, h] = jnp.zeros((HEAD + EXTRA, rows), f32)
        top[i, h] = jnp.full((8, rows), NEG, f32)

    with jax.named_scope("own_pair"):
        lax.fori_loop(0, n * heads, clear, None)
        pair(me, me, True)

    with jax.named_scope("wait_g1"):
        for i in range(SUB):
            for way in range(2):
                ag(way, 0, i).wait_recv()
                ag(way, 2, i).start()
    with jax.named_scope("proj_g1"):
        project_kv(1)
        project_q(1)
    with jax.named_scope("wait_g2"):
        for i in range(SUB):
            for way in range(2):
                ag(way, 1, i).wait_recv()
    with jax.named_scope("proj_g2"):
        project_kv(2)
        project_q(2)
    with jax.named_scope("pairs_early"):
        pairs(lambda i, j: (i != opp) & (j != opp) & ((i != me) | (j != me)))

    for part in range(2):
        with jax.named_scope("wait_g3"):
            for i in range(part * SUB // 2, (part + 1) * SUB // 2):
                for way in range(2):
                    ag(way, 2, i).wait_recv()
        with jax.named_scope("kv_g3"):
            project_kv(3, part)
        with jax.named_scope("pairs_sides"):

            def sides(t, _):
                i = jnp.where(t == 0, right, left)

                @pl.when(i > opp)
                def _():
                    pair(i, opp, False, part)

            lax.fori_loop(0, 2, sides, None)
    with jax.named_scope("finish_sides"):
        finish(right)
        finish(left)

    def rs(way, leg, c):
        return pltpu.make_async_remote_copy(
            src_ref=sbuf.at[way, leg * nc + c],
            dst_ref=rbuf.at[way, leg * nc + c],
            send_sem=rs_send.at[way, leg * nc + c],
            recv_sem=rs_recv.at[way, leg * nc + c],
            device_id={"tp": (right, left)[way]},
            device_id_type=pl.DeviceIdType.MESH,
        )

    def attended(b):
        return q[pl.ds(pl.multiple_of(b * rows, rows), rows), :]

    def tiles(leg, c):
        step = leg * nc + c

        @pl.when(step + DEPTH - 1 < 4 * nc)
        def _():
            for s in range(2):
                wo_copy(step + DEPTH - 1, s).start()

        for s in range(2):
            wo_copy(step, s).wait()
        return lax.rem(step, DEPTH)

    def leg0(c, _):
        slot = tiles(0, c)
        sbuf[0, c] = _dot(attended(right), wob[slot, 1]).astype(bf16)
        sbuf[1, c] = _dot(attended(left), wob[slot, 0]).astype(bf16)
        rs(0, 0, c).start()
        rs(1, 0, c).start()

    def leg1(c, _):
        slot = tiles(1, c)
        for way in range(2):
            sbuf[way, nc + c] = _dot(attended(opp), wob[slot, way]).astype(bf16)
        for way in range(2):
            rs(way, 1, c).start()

    def leg2(c, _):
        slot = tiles(2, c)
        for way, b in enumerate((right, left)):
            term = _dot(attended(b), wob[slot, way])
            rs(way, 1, c).wait_recv()
            sbuf[way, 2 * nc + c] = (term + rbuf[way, nc + c].astype(f32)).astype(bf16)
            rs(way, 2, c).start()

    def leg3(c, _):
        slot = tiles(3, c)
        for s in range(2):
            at = pl.ds(pl.multiple_of(s * hw + c * CW, CW), CW)
            term = _dot(attended(me), wob[slot, s]) + y_ref[:, at].astype(f32)
            rs(1 - s, 0, c).wait_recv()
            term += rbuf[1 - s, c].astype(f32)
            rs(s, 2, c).wait_recv()
            y_ref[:, at] = (term + rbuf[s, 2 * nc + c].astype(f32)).astype(bf16)

    with jax.named_scope("leg0"):
        lax.fori_loop(0, nc, leg0, None)
    with jax.named_scope("q_g3"):
        project_q(3)
    with jax.named_scope("pairs_opp"):
        pairs(lambda i, j: (i == opp) | ((j == opp) & (i == me)))
        finish(opp)
    with jax.named_scope("leg1"):
        lax.fori_loop(0, nc, leg1, None)
    with jax.named_scope("leg2"):
        finish(me)
        lax.fori_loop(0, nc, leg2, None)
    with jax.named_scope("leg3"):
        lax.fori_loop(0, nc, leg3, None)

    for way in range(2):
        for leg in range(3):
            for i in range(SUB):
                ag(way, leg, i).wait_send()

    def drain(c, _):
        for way in range(2):
            for leg in range(3):
                rs(way, leg, c).wait_send()

    lax.fori_loop(0, nc, drain, None)


def _table(tokens):
    half = HEAD // 2
    angle = np.arange(tokens, dtype=np.float64)[:, None] * float(THETA) ** (-np.arange(half, dtype=np.float64) / half)
    return np.concatenate([np.cos(angle), np.sin(angle)], -1).astype(np.float32)


def solution(mesh):
    n = mesh.shape["tp"]

    def step(x, gain, wq, wk, wv, wo):
        rows, width = x.shape
        tokens, qwidth = n * rows, wq.shape[1]
        heads = qwidth // HEAD
        nc = width // 2 // CW
        bf16, f32 = jnp.bfloat16, jnp.float32
        dma = pltpu.SemaphoreType.DMA
        hbm = pl.BlockSpec(memory_space=pl.ANY)
        return pl.pallas_call(
            functools.partial(_kernel, n),
            out_shape=pltpu.VMEM((rows, width), bf16),
            in_specs=[hbm] * 7,
            out_specs=pl.BlockSpec(memory_space=pltpu.VMEM),
            scratch_shapes=[
                pltpu.VMEM((width,), bf16),
                pltpu.VMEM((tokens, width), bf16),
                pltpu.VMEM((width, qwidth), bf16),
                pltpu.VMEM((width, 2 * HEAD), bf16),
                pltpu.VMEM((tokens, HEAD), f32),
                pltpu.VMEM((tokens, qwidth), bf16),
                pltpu.VMEM((tokens, HEAD), bf16),
                pltpu.VMEM((tokens, HEAD), bf16),
                pltpu.VMEM((n, heads, HEAD + EXTRA, rows), f32),
                pltpu.VMEM((n, heads, 8, rows), f32),
                pltpu.VMEM((DEPTH, 2, qwidth, CW), bf16),
                pltpu.VMEM((2, 3 * nc, rows, CW), bf16),
                pltpu.VMEM((2, 3 * nc, rows, CW), bf16),
                dma((2 * SUB,)), dma, dma((qwidth // QT,)), dma((3,)), dma((DEPTH, 2)),
                dma((2, 3, SUB)), dma((2, 3, SUB)), dma((2, 3 * nc)), dma((2, 3 * nc)),
            ],
            compiler_params=pltpu.CompilerParams(collective_id=0, has_side_effects=True, vmem_limit_bytes=VMEM),
        )(x, gain, wq, wk, wv, wo, _table(tokens))

    tokens, columns = P(("dp", "tp"), None), P(None, "tp")
    return jax.shard_map(
        step,
        mesh=mesh,
        in_specs=(tokens, P(None), columns, columns, columns, P("tp", None)),
        out_specs=tokens,
        check_vma=False,
    )
```

```python
import functools

import jax
import jax.numpy as jnp
import numpy as np
from jax import lax
from jax.experimental import pallas as pl
from jax.experimental.pallas import tpu as pltpu
from jax.sharding import PartitionSpec as P

HEAD = 128
THETA = 10000
NEG = -1e30
HIDDEN = 2 * NEG
LOG2E = 1.4426950408889634
SUB = 4
QT = 256
CW = 256
FINISH = 8
UNROLL = 8
DEPTH = 3
VMEM = 61 * 2**20 + 2**19
EXTRA = 16


def _dot(a, b, ca=1, cb=0):
    return lax.dot_general(a, b, (((ca,), (cb,)), ((), ())), preferred_element_type=jnp.float32)


def _kernel(n, x_ref, gain_ref, wq_ref, wk_ref, wv_ref, wo_ref, tab_ref, y_ref,
            gs, xg, wq, wkv, tab, q, k, v, mix, top, wob, sbuf, rbuf,
            x_sem, g_sem, wq_sem, w_sem, wo_sem, ag_send, ag_recv, rs_send, rs_recv):
    rows, width = x_ref.shape
    half = rows // 2
    sub = half // SUB
    qwidth = wq_ref.shape[1]
    heads = qwidth // HEAD
    hw = width // 2
    nc = hw // CW
    qn = qwidth // QT
    bf16, f32 = jnp.bfloat16, jnp.float32

    me = lax.axis_index("tp")
    right, left, opp = lax.rem(me + 1, n), lax.rem(me + n - 1, n), lax.rem(me + 2, n)

    X_CUTS = (0, 1, 2, 4, 2 * SUB)

    def x_copy(i):
        at = pl.ds(X_CUTS[i] * sub, (X_CUTS[i + 1] - X_CUTS[i]) * sub)
        return pltpu.make_async_copy(x_ref.at[at], y_ref.at[at], x_sem.at[i])

    def wq_copy(i):
        at = pl.ds(pl.multiple_of(i * 2 * QT, 2 * QT), 2 * QT)
        return pltpu.make_async_copy(wq_ref.at[:, at], wq.at[:, at], wq_sem.at[i])

    def wo_copy(step, s):
        c = lax.rem(step, nc)
        slot = lax.rem(step, DEPTH)
        return pltpu.make_async_copy(wo_ref.at[:, pl.ds(pl.multiple_of(s * hw + c * CW, CW), CW)], wob.at[slot, s], wo_sem.at[slot])

    def wo_both(slot):
        return pltpu.make_async_copy(wob.at[slot], wob.at[slot], wo_sem.at[slot])

    g_copy = pltpu.make_async_copy(gain_ref, gs, g_sem)
    tab_copy = pltpu.make_async_copy(tab_ref, tab, w_sem.at[2])
    wk_copy = pltpu.make_async_copy(wk_ref, wkv.at[:, pl.ds(0, HEAD)], w_sem.at[0])
    wv_copy = pltpu.make_async_copy(wv_ref, wkv.at[:, pl.ds(HEAD, HEAD)], w_sem.at[1])

    barrier = pltpu.get_barrier_semaphore()
    for neighbour in (left, right):
        pl.semaphore_signal(barrier, inc=1, device_id={"tp": neighbour}, device_id_type=pl.DeviceIdType.MESH)
    g_copy.start()
    for i in range(len(X_CUTS) - 1):
        x_copy(i).start()

    def source(way, leg, i):
        if leg < 2:
            return (2 * i + (leg if way == 0 else 1 - leg)) * sub
        return rows + way * half + i * sub

    def target(way, leg, i):
        if leg < 2:
            return (leg + 1) * rows + way * half + i * sub
        return 3 * rows + (2 * i + way) * sub

    def ag(way, leg, i):
        return pltpu.make_async_remote_copy(
            src_ref=xg.at[pl.ds(source(way, leg, i), sub)],
            dst_ref=xg.at[pl.ds(target(way, leg, i), sub)],
            send_sem=ag_send.at[way, leg],
            recv_sem=ag_recv.at[way, leg if leg < 2 else 2 + i // (SUB // 2)],
            device_id={"tp": (right, left)[way]},
            device_id_type=pl.DeviceIdType.MESH,
        )

    def ag_all(way, leg, part=None):
        at = pl.ds((min(leg, 1) * 2 + way) * half, half if part is None else half // 2)
        return pltpu.make_async_remote_copy(
            src_ref=xg.at[at],
            dst_ref=xg.at[at],
            send_sem=ag_send.at[way, leg],
            recv_sem=ag_recv.at[way, leg if leg < 2 else 2 + (part or 0)],
            device_id={"tp": (right, left)[way]},
            device_id_type=pl.DeviceIdType.MESH,
        )

    step16 = 16

    def norm(start, count):
        def body(t, _):
            at = pl.ds(pl.multiple_of(start + t * step16, step16), step16)
            wide = y_ref[at, :].astype(f32)
            scale = lax.rsqrt(jnp.mean(wide * wide, -1, keepdims=True) + 1e-6)
            xg[at, :] = (wide * scale * gs[...].astype(f32)[None, :]).astype(bf16)

        lax.fori_loop(0, count // step16, body, None)

    with jax.named_scope("norm"):
        g_copy.wait()
        for i in range(SUB):
            for p in range(2):
                if 2 * i + p in X_CUTS:
                    x_copy(X_CUTS.index(2 * i + p)).wait()
                if 2 * i + p == X_CUTS[-2]:
                    wk_copy.start()
                    wv_copy.start()
                    tab_copy.start()
                    for j in range(qn // 2):
                        wq_copy(j).start()
                norm((2 * i + p) * sub, sub)
                if i == 0 and p == 0:
                    pl.semaphore_wait(barrier, 2)
                ag(p, 0, i).start()
        for way, late in ((0, 1), (1, 3)):

            @pl.when(me != late)
            def _(way=way):
                for i in range(SUB):
                    ag(way, 1, i).start()

        for ahead in range(DEPTH - 1):
            for s in range(2):
                wo_copy(ahead, s).start()

    lane = lax.broadcasted_iota(jnp.int32, (1, HEAD), 1)
    low = lane < HEAD // 2

    def turn(t, at):
        cs = tab[pl.ds(pl.multiple_of(at, sub), t.shape[0]), :]
        sc = pltpu.roll(cs, HEAD // 2, 1)
        t = t.astype(f32)
        return (t * jnp.where(low, cs, sc) + pltpu.roll(t, HEAD // 2, 1) * jnp.where(low, -sc, cs)).astype(bf16)

    def runs(g):
        if g in (0, 3):
            return ((0, rows, (me if g == 0 else opp) * rows),)
        halves = ((left, 0), (right, 1)) if g == 1 else ((left, 1), (right, 0))
        return tuple((p * half + i * sub, sub, b * rows + (2 * i + h) * sub) for p, (b, h) in enumerate(halves) for i in range(SUB))

    def project_kv(g, part=None):
        first, count = (0, rows) if part is None else (part * half, half)
        t = _dot(xg[pl.ds(g * rows + first, count), :], wkv[...]).astype(bf16)
        for row, size, at in runs(g) if part is None else ((0, half, runs(g)[0][2] + first),):
            at = pl.multiple_of(at, sub)
            k[pl.ds(at, size), :] = turn(t[row : row + size, :HEAD], at)
            v[pl.ds(at, size), :] = t[row : row + size, HEAD:]

    def project_q(g):
        def body(j, _):
            if g == 0:

                @pl.when(lax.rem(j, 2) == 0)
                def _():
                    wq_copy(j // 2).wait()

            t = _dot(xg[pl.ds(g * rows, rows), :], wq[:, pl.ds(pl.multiple_of(j * QT, QT), QT)]).astype(bf16)
            for row, size, at in runs(g):
                at = pl.multiple_of(at, sub)
                for e in range(QT // HEAD):
                    part = t[row : row + size, e * HEAD : (e + 1) * HEAD]
                    q[pl.ds(at, size), pl.ds(pl.multiple_of(j * QT + e * HEAD, HEAD), HEAD)] = turn(part, at)

        lax.fori_loop(0, qn, body, None)

    e2 = HEAD**-0.5 * LOG2E

    def pair(i, j, masked, part=None):
        first, count = (0, rows) if part is None else (part * half, half)
        keys = pl.ds(pl.multiple_of(j * rows + first, half), count)
        kj = k[keys, :]
        vj = jnp.concatenate([v[keys, :].astype(f32).T.astype(bf16), jnp.ones((EXTRA, count), bf16)], axis=0)
        if masked:
            ok = lax.broadcasted_iota(jnp.int32, (rows, rows), 0) <= lax.broadcasted_iota(jnp.int32, (rows, rows), 1)

        unroll = UNROLL if part is None else 2 * UNROLL

        def body(m, _):
            hs = [m * unroll + u for u in range(unroll)]
            scores = [_dot(kj, q[pl.ds(pl.multiple_of(i * rows, rows), rows), pl.ds(pl.multiple_of(h * HEAD, HEAD), HEAD)], 1, 1) for h in hs]
            weights, keeps = [], []
            for h, s in zip(hs, scores):
                if masked:
                    s = jnp.where(ok, s, HIDDEN)
                old = top[i, h, 0:1, :]
                new = jnp.maximum(old, s.max(axis=0, keepdims=True))
                top[i, h, 0:1, :] = new
                weights.append(jnp.exp2((s - new) * e2).astype(bf16))
                keeps.append(jnp.exp2((old - new) * e2))
            for h, p, keep in zip(hs, weights, keeps):
                mix[i, h] = mix[i, h] * keep + _dot(vj, p)

        lax.fori_loop(0, heads // unroll, body, None)

    def pairs(wanted):
        def body(t, _):
            i, j = t // n, lax.rem(t, n)

            @pl.when((i > j) & wanted(i, j))
            def _():
                pair(i, j, False)

            @pl.when((i == j) & wanted(i, j))
            def _():
                pair(i, j, True)

        lax.fori_loop(0, n * n, body, None)

    def finish(i):
        def body(m, _):
            for u in range(FINISH):
                h = m * FINISH + u
                out = mix[i, h, :HEAD, :] * (1 / mix[i, h, HEAD : HEAD + 1, :])
                q[pl.ds(pl.multiple_of(i * rows, rows), rows), pl.ds(pl.multiple_of(h * HEAD, HEAD), HEAD)] = out.T.astype(bf16)

        lax.fori_loop(0, heads // FINISH, body, None)

    with jax.named_scope("own_proj"):
        tab_copy.wait()
        wk_copy.wait()
        wv_copy.wait()
        project_kv(0)
        project_q(0)

    def clear(t, _):
        i, h = t // heads, lax.rem(t, heads)
        mix[i, h] = jnp.zeros((HEAD + EXTRA, rows), f32)
        top[i, h] = jnp.full((8, rows), NEG, f32)

    with jax.named_scope("own_pair"):
        lax.fori_loop(0, n * heads, clear, None)
        pair(me, me, True)

    special = opp == 0

    def known(b):
        return (b == me) | ((b == opp) == special)

    def wait_ag(leg, *parts):
        for part in parts or (None,):
            for way in range(2):
                ag_all(way, leg, part).wait_recv()

    with jax.named_scope("wait_g1"):
        wait_ag(0)
        for i in range(SUB):
            for way in range(2):
                ag(way, 2, i).start()
        for way, late in ((0, 1), (1, 3)):

            @pl.when(me == late)
            def _(way=way):
                for i in range(SUB):
                    ag(way, 1, i).start()

    with jax.named_scope("proj_g1"):
        project_kv(1)
        project_q(1)

    @pl.when(jnp.logical_not(special))
    def _():
        with jax.named_scope("wait_g2"):
            wait_ag(1)
        with jax.named_scope("proj_g2"):
            project_kv(2)
            project_q(2)

    @pl.when(special)
    def _():
        with jax.named_scope("wait_g3"):
            wait_ag(2, 0, 1)
        with jax.named_scope("proj_g3"):
            project_kv(3)
            project_q(3)

    with jax.named_scope("pairs_early"):
        pairs(lambda i, j: known(i) & known(j) & ((i != me) | (j != me)))

    def finishes(wanted):
        def body(b, _):
            @pl.when(wanted(b))
            def _():
                finish(b)

        lax.fori_loop(0, n, body, None)

    def rs(way, leg, c):
        return pltpu.make_async_remote_copy(
            src_ref=sbuf.at[way, lax.rem(leg, 2) * nc + c],
            dst_ref=rbuf.at[way, leg * nc + c],
            send_sem=rs_send.at[way, leg],
            recv_sem=rs_recv.at[way, jnp.where(leg == 0, 0, 1 + (leg - 1) * nc + c)],
            device_id={"tp": (right, left)[way]},
            device_id_type=pl.DeviceIdType.MESH,
        )

    def rs_all(way, leg):
        return pltpu.make_async_remote_copy(
            src_ref=sbuf.at[way, pl.ds(leg % 2 * nc, nc)],
            dst_ref=rbuf.at[way, pl.ds(leg * nc, nc)],
            send_sem=rs_send.at[way, leg],
            recv_sem=rs_recv.at[way, 0],
            device_id={"tp": (right, left)[way]},
            device_id_type=pl.DeviceIdType.MESH,
        )

    def attended(b):
        return q[pl.ds(pl.multiple_of(b * rows, rows), rows), :]

    def tiles(leg, c):
        step = leg * nc + c

        @pl.when(step + DEPTH - 1 < 4 * nc)
        def _():
            for s in range(2):
                wo_copy(step + DEPTH - 1, s).start()

        slot = lax.rem(step, DEPTH)
        wo_both(slot).wait()
        return slot

    def send_terms(leg, turn):
        aims = (jnp.where(leg == 0, right, opp), jnp.where(leg == 0, left, opp))

        def body(c, _):
            slot = tiles(turn, c)
            for way in range(2):
                side = (1 - leg, leg)[way]
                sbuf[way, leg * nc + c] = _dot(attended(aims[way]), wob[slot, side]).astype(bf16)
            for way in range(2):
                rs(way, leg, c).start()

        lax.fori_loop(0, nc, body, None)

    def leg2(c, _):
        slot = tiles(2, c)
        terms = [_dot(attended(b), wob[slot, way]) for way, b in enumerate((right, left))]
        for way in range(2):
            rs(way, 1, c).wait_recv()
            sbuf[way, c] = (terms[way] + rbuf[way, nc + c].astype(f32)).astype(bf16)
        for way in range(2):
            rs(way, 2, c).start()

    def leg3(c, _):
        slot = tiles(3, c)
        at = [pl.ds(pl.multiple_of(s * hw + c * CW, CW), CW) for s in range(2)]
        terms = [_dot(attended(me), wob[slot, s]) + y_ref[:, at[s]].astype(f32) for s in range(2)]
        for s in range(2):
            terms[s] += rbuf[1 - s, c].astype(f32)
        for s in range(2):
            rs(s, 2, c).wait_recv()
            y_ref[:, at[s]] = (terms[s] + rbuf[s, 2 * nc + c].astype(f32)).astype(bf16)

    with jax.named_scope("finish_early"):
        finishes(lambda b: jnp.where(special, b == opp, (b != me) & (b < opp)))

    @pl.when((me == 1) | special)
    def _():
        with jax.named_scope("leg_early"):
            send_terms(jnp.where(special, 1, 0), 0)

    @pl.when(jnp.logical_not(special))
    def _():
        for part in range(2):
            with jax.named_scope("wait_g3"):
                wait_ag(2, part)
            with jax.named_scope("kv_g3"):
                project_kv(3, part)
            with jax.named_scope("pairs_sides"):

                def sides(t, _):
                    i = jnp.where(t == 0, right, left)

                    @pl.when(i > opp)
                    def _():
                        pair(i, opp, False, part)

                lax.fori_loop(0, 2, sides, None)

    @pl.when(special)
    def _():
        with jax.named_scope("wait_g2"):
            wait_ag(1)
        with jax.named_scope("proj_g2"):
            project_kv(2)
            project_q(2)
        with jax.named_scope("pairs_sides"):
            pairs(lambda i, j: (i != me) & (i != opp))

    with jax.named_scope("finish_sides"):
        finishes(lambda b: (b != me) & (b != opp) & (special | (b > opp)))

    @pl.when(me != 1)
    def _():
        with jax.named_scope("leg0"):
            send_terms(0, jnp.where(special, 1, 0))

    @pl.when(jnp.logical_not(special))
    def _():
        with jax.named_scope("q_g3"):
            project_q(3)

    with jax.named_scope("pairs_opp"):
        pairs(lambda i, j: ((i == me) & jnp.logical_not(known(j))) | ((i == opp) & jnp.logical_not(special)))

    @pl.when(jnp.logical_not(special))
    def _():
        with jax.named_scope("leg1"):
            finish(opp)
            send_terms(1, 1)

    for way in range(2):
        for leg in range(3):
            ag_all(way, leg).wait_send()
    with jax.named_scope("leg2"):
        finish(me)
        for way in range(2):
            rs_all(way, 0).wait_send()
        lax.fori_loop(0, nc, leg2, None)
    with jax.named_scope("leg3"):
        for way in range(2):
            rs_all(way, 0).wait_recv()
        lax.fori_loop(0, nc, leg3, None)
    with jax.named_scope("drain"):
        for way in range(2):
            for leg in (1, 2):
                rs_all(way, leg).wait_send()


def _table(tokens):
    half = HEAD // 2
    angle = np.arange(tokens, dtype=np.float64)[:, None] * float(THETA) ** (-np.arange(half, dtype=np.float64) / half)
    return np.concatenate([np.cos(angle), np.sin(angle)], -1).astype(np.float32)


def solution(mesh):
    n = mesh.shape["tp"]

    def step(x, gain, wq, wk, wv, wo):
        rows, width = x.shape
        tokens, qwidth = n * rows, wq.shape[1]
        heads = qwidth // HEAD
        nc = width // 2 // CW
        bf16, f32 = jnp.bfloat16, jnp.float32
        dma = pltpu.SemaphoreType.DMA
        hbm = pl.BlockSpec(memory_space=pl.ANY)
        return pl.pallas_call(
            functools.partial(_kernel, n),
            out_shape=pltpu.VMEM((rows, width), bf16),
            in_specs=[hbm] * 7,
            out_specs=pl.BlockSpec(memory_space=pltpu.VMEM),
            scratch_shapes=[
                pltpu.VMEM((width,), bf16),
                pltpu.VMEM((tokens, width), bf16),
                pltpu.VMEM((width, qwidth), bf16),
                pltpu.VMEM((width, 2 * HEAD), bf16),
                pltpu.VMEM((tokens, HEAD), f32),
                pltpu.VMEM((tokens, qwidth), bf16),
                pltpu.VMEM((tokens, HEAD), bf16),
                pltpu.VMEM((tokens, HEAD), bf16),
                pltpu.VMEM((n, heads, HEAD + EXTRA, rows), f32),
                pltpu.VMEM((n, heads, 8, rows), f32),
                pltpu.VMEM((DEPTH, 2, qwidth, CW), bf16),
                pltpu.VMEM((2, 2 * nc, rows, CW), bf16),
                pltpu.VMEM((2, 3 * nc, rows, CW), bf16),
                dma((4,)), dma, dma((qwidth // QT // 2,)), dma((3,)), dma((DEPTH,)),
                dma((2, 3)), dma((2, 4)), dma((2, 3)), dma((2, 1 + 2 * nc)),
            ],
            compiler_params=pltpu.CompilerParams(collective_id=0, has_side_effects=True, vmem_limit_bytes=VMEM),
        )(x, gain, wq, wk, wv, wo, _table(tokens))

    tokens, columns = P(("dp", "tp"), None), P(None, "tp")
    return jax.shard_map(
        step,
        mesh=mesh,
        in_specs=(tokens, P(None), columns, columns, columns, P("tp", None)),
        out_specs=tokens,
        check_vma=False,
    )
```

```python
import functools

import jax
import jax.numpy as jnp
import numpy as np
from jax import lax
from jax.experimental import pallas as pl
from jax.experimental.pallas import tpu as pltpu
from jax.sharding import PartitionSpec as P

HEAD = 128
THETA = 10000
NEG = -1e30
HIDDEN = 2 * NEG
LOG2E = 1.4426950408889634
SUB = 4
QT = 256
CW = 256
FINISH = 8
UNROLL = 8
DEPTH = 3
VMEM = 61 * 2**20 + 2**19
EXTRA = 16


def _dot(a, b, ca=1, cb=0):
    return lax.dot_general(a, b, (((ca,), (cb,)), ((), ())), preferred_element_type=jnp.float32)


def _kernel(n, x_ref, gain_ref, wq_ref, wk_ref, wv_ref, wo_ref, tab_ref, y_ref,
            gs, xg, wq, wkv, tab, q, k, v, mix, top, wob, sbuf, rbuf,
            x_sem, g_sem, wq_sem, w_sem, wo_sem, ag_send, ag_recv, rs_send, rs_recv):
    rows, width = x_ref.shape
    half = rows // 2
    sub = half // SUB
    qwidth = wq_ref.shape[1]
    heads = qwidth // HEAD
    hw = width // 2
    nc = hw // CW
    qn = qwidth // QT
    bf16, f32 = jnp.bfloat16, jnp.float32

    me = lax.axis_index("tp")
    right, left, opp = lax.rem(me + 1, n), lax.rem(me + n - 1, n), lax.rem(me + 2, n)

    X_CUTS = (0, 1, 2, 4, 2 * SUB)

    def x_copy(i):
        at = pl.ds(X_CUTS[i] * sub, (X_CUTS[i + 1] - X_CUTS[i]) * sub)
        return pltpu.make_async_copy(x_ref.at[at], y_ref.at[at], x_sem.at[i])

    def wq_copy(i):
        at = pl.ds(pl.multiple_of(i * 2 * QT, 2 * QT), 2 * QT)
        return pltpu.make_async_copy(wq_ref.at[:, at], wq.at[:, at], wq_sem.at[i])

    def wo_copy(step, s):
        c = lax.rem(step, nc)
        slot = lax.rem(step, DEPTH)
        return pltpu.make_async_copy(wo_ref.at[:, pl.ds(pl.multiple_of(s * hw + c * CW, CW), CW)], wob.at[slot, s], wo_sem.at[slot, s])

    split = (me == 0) | (me == 3)
    more = jnp.where(split, 1, 0)

    def fetch(step):
        for s in range(2):

            @pl.when((step < (4 + more) * nc) & jnp.logical_not(split & (step < 2 * nc) & ((step // (nc // 2) % 3 == 0) == (s == 0))))
            def _(s=s):
                wo_copy(step, s).start()

    g_copy = pltpu.make_async_copy(gain_ref, gs, g_sem)
    tab_copy = pltpu.make_async_copy(tab_ref, tab, w_sem.at[2])
    wk_copy = pltpu.make_async_copy(wk_ref, wkv.at[:, pl.ds(0, HEAD)], w_sem.at[0])
    wv_copy = pltpu.make_async_copy(wv_ref, wkv.at[:, pl.ds(HEAD, HEAD)], w_sem.at[1])

    barrier = pltpu.get_barrier_semaphore()
    for neighbour in (left, right):
        pl.semaphore_signal(barrier, inc=1, device_id={"tp": neighbour}, device_id_type=pl.DeviceIdType.MESH)
    g_copy.start()
    for i in range(len(X_CUTS) - 1):
        x_copy(i).start()

    def source(way, leg, i):
        if leg < 2:
            return (2 * i + (leg if way == 0 else 1 - leg)) * sub
        return rows + way * half + i * sub

    def target(way, leg, i):
        if leg == 0:
            return rows + way * half + i * sub
        if leg == 1:
            return 2 * rows + i // (SUB // 2) * half + way * (half // 2) + i % (SUB // 2) * sub
        return 3 * rows + (2 * i + way) * sub

    def arrival(leg, part):
        return 0 if leg == 0 else 2 * leg - 1 + part

    def ag(way, leg, i):
        return pltpu.make_async_remote_copy(
            src_ref=xg.at[pl.ds(source(way, leg, i), sub)],
            dst_ref=xg.at[pl.ds(target(way, leg, i), sub)],
            send_sem=ag_send.at[way, leg],
            recv_sem=ag_recv.at[way, arrival(leg, i // (SUB // 2))],
            device_id={"tp": (right, left)[way]},
            device_id_type=pl.DeviceIdType.MESH,
        )

    def ag_all(way, leg, part=None):
        at = pl.ds((min(leg, 1) * 2 + way) * half, half if part is None else half // 2)
        return pltpu.make_async_remote_copy(
            src_ref=xg.at[at],
            dst_ref=xg.at[at],
            send_sem=ag_send.at[way, leg],
            recv_sem=ag_recv.at[way, arrival(leg, part or 0)],
            device_id={"tp": (right, left)[way]},
            device_id_type=pl.DeviceIdType.MESH,
        )

    step16 = 16

    def norm(start, count):
        def body(t, _):
            at = pl.ds(pl.multiple_of(start + t * step16, step16), step16)
            wide = y_ref[at, :].astype(f32)
            scale = lax.rsqrt(jnp.mean(wide * wide, -1, keepdims=True) + 1e-6)
            xg[at, :] = (wide * scale * gs[...].astype(f32)[None, :]).astype(bf16)

        lax.fori_loop(0, count // step16, body, None)

    with jax.named_scope("norm"):
        g_copy.wait()
        for i in range(SUB):
            for p in range(2):
                if 2 * i + p in X_CUTS:
                    x_copy(X_CUTS.index(2 * i + p)).wait()
                if 2 * i + p == X_CUTS[-2]:
                    wk_copy.start()
                    wv_copy.start()
                    tab_copy.start()
                    for j in range(qn // 2):
                        wq_copy(j).start()
                norm((2 * i + p) * sub, sub)
                if i == 0 and p == 0:
                    pl.semaphore_wait(barrier, 2)
                ag(p, 0, i).start()
        for way, late in ((0, 1), (1, 3)):

            @pl.when(me != late)
            def _(way=way):
                for i in range(SUB):
                    ag(way, 1, i).start()

        for ahead in range(DEPTH - 1):
            fetch(ahead)

    lane = lax.broadcasted_iota(jnp.int32, (1, HEAD), 1)
    low = lane < HEAD // 2

    def turn(t, at):
        cs = tab[pl.ds(pl.multiple_of(at, sub), t.shape[0]), :]
        sc = pltpu.roll(cs, HEAD // 2, 1)
        t = t.astype(f32)
        return (t * jnp.where(low, cs, sc) + pltpu.roll(t, HEAD // 2, 1) * jnp.where(low, -sc, cs)).astype(bf16)

    def runs(g):
        if g in (0, 3):
            return ((0, rows, (me if g == 0 else opp) * rows),)
        if g == 1:
            return tuple((p * half + i * sub, sub, b * rows + (2 * i + p) * sub) for p, b in enumerate((left, right)) for i in range(SUB))
        return tuple((target(p, 1, i) - 2 * rows, sub, b * rows + (2 * i + 1 - p) * sub) for i in range(SUB) for p, b in enumerate((left, right)))

    def rows_of(g, part):
        if part is None:
            return 0, rows, runs(g)
        first = part * half
        if g == 3:
            return first, half, ((0, half, runs(3)[0][2] + first),)
        return first, half, tuple((row - first, size, at) for row, size, at in runs(g) if first <= row < first + half)

    def project_kv(g, part=None):
        first, count, pieces = rows_of(g, part)
        t = _dot(xg[pl.ds(g * rows + first, count), :], wkv[...]).astype(bf16)
        for row, size, at in pieces:
            at = pl.multiple_of(at, sub)
            k[pl.ds(at, size), :] = turn(t[row : row + size, :HEAD], at)
            v[pl.ds(at, size), :] = t[row : row + size, HEAD:]

    def project_q(g, part=None):
        first, count, pieces = rows_of(g, part)

        def body(j, _):
            if g == 0:

                @pl.when(lax.rem(j, 2) == 0)
                def _():
                    wq_copy(j // 2).wait()

            t = _dot(xg[pl.ds(g * rows + first, count), :], wq[:, pl.ds(pl.multiple_of(j * QT, QT), QT)]).astype(bf16)
            for row, size, at in pieces:
                at = pl.multiple_of(at, sub)
                for e in range(QT // HEAD):
                    part_ = t[row : row + size, e * HEAD : (e + 1) * HEAD]
                    q[pl.ds(at, size), pl.ds(pl.multiple_of(j * QT + e * HEAD, HEAD), HEAD)] = turn(part_, at)

        lax.fori_loop(0, qn, body, None)

    e2 = HEAD**-0.5 * LOG2E

    def pair(i, j, masked, part=None):
        first, count = (0, rows) if part is None else (part * half, half)
        keys = pl.ds(pl.multiple_of(j * rows + first, half), count)
        kj = k[keys, :]
        vj = jnp.concatenate([v[keys, :].astype(f32).T.astype(bf16), jnp.ones((EXTRA, count), bf16)], axis=0)
        if masked:
            ok = lax.broadcasted_iota(jnp.int32, (rows, rows), 0) <= lax.broadcasted_iota(jnp.int32, (rows, rows), 1)

        unroll = UNROLL if part is None else 2 * UNROLL

        def body(m, _):
            hs = [m * unroll + u for u in range(unroll)]
            scores = [_dot(kj, q[pl.ds(pl.multiple_of(i * rows, rows), rows), pl.ds(pl.multiple_of(h * HEAD, HEAD), HEAD)], 1, 1) for h in hs]
            weights, keeps = [], []
            for h, s in zip(hs, scores):
                if masked:
                    s = jnp.where(ok, s, HIDDEN)
                old = top[i, h, 0:1, :]
                new = jnp.maximum(old, s.max(axis=0, keepdims=True))
                top[i, h, 0:1, :] = new
                weights.append(jnp.exp2((s - new) * e2).astype(bf16))
                keeps.append(jnp.exp2((old - new) * e2))
            for h, p, keep in zip(hs, weights, keeps):
                mix[i, h] = mix[i, h] * keep + _dot(vj, p)

        lax.fori_loop(0, heads // unroll, body, None)

    def pairs(wanted):
        def body(t, _):
            i, j = t // n, lax.rem(t, n)

            @pl.when((i > j) & wanted(i, j))
            def _():
                pair(i, j, False)

            @pl.when((i == j) & wanted(i, j))
            def _():
                pair(i, j, True)

        lax.fori_loop(0, n * n, body, None)

    def finish(i):
        def body(m, _):
            for u in range(FINISH):
                h = m * FINISH + u
                out = mix[i, h, :HEAD, :] * (1 / mix[i, h, HEAD : HEAD + 1, :])
                q[pl.ds(pl.multiple_of(i * rows, rows), rows), pl.ds(pl.multiple_of(h * HEAD, HEAD), HEAD)] = out.T.astype(bf16)

        lax.fori_loop(0, heads // FINISH, body, None)

    with jax.named_scope("own_proj"):
        tab_copy.wait()
        wk_copy.wait()
        wv_copy.wait()
        project_kv(0)
        project_q(0)

    def clear(t, _):
        i, h = t // heads, lax.rem(t, heads)
        mix[i, h] = jnp.zeros((HEAD + EXTRA, rows), f32)
        top[i, h] = jnp.full((8, rows), NEG, f32)

    with jax.named_scope("own_pair"):
        lax.fori_loop(0, n * heads, clear, None)
        pair(me, me, True)

    special = opp == 0

    def known(b):
        return (b == me) | ((b == opp) == special)

    def wait_ag(leg, *parts):
        for part in parts or (None,):
            for way in range(2):
                ag_all(way, leg, part).wait_recv()

    with jax.named_scope("wait_g1"):
        wait_ag(0)
        for i in range(SUB):
            for way in range(2):
                ag(way, 2, i).start()
        for way, late in ((0, 1), (1, 3)):

            @pl.when(me == late)
            def _(way=way):
                for i in range(SUB):
                    ag(way, 1, i).start()

    with jax.named_scope("proj_g1"):
        project_kv(1)
        project_q(1)

    @pl.when(jnp.logical_not(special))
    def _():
        for part in range(2):
            with jax.named_scope("wait_g2"):
                wait_ag(1, part)
            with jax.named_scope("proj_g2"):
                project_kv(2, part)
                project_q(2, part)

    @pl.when(special)
    def _():
        for part in range(2):
            with jax.named_scope("wait_g3"):
                wait_ag(2, part)
            with jax.named_scope("proj_g3"):
                project_kv(3, part)
                project_q(3, part)

    with jax.named_scope("pairs_early"):
        pairs(lambda i, j: known(i) & known(j) & (i != me))

    def finishes(wanted):
        def body(b, _):
            @pl.when(wanted(b))
            def _():
                finish(b)

        lax.fori_loop(0, n, body, None)

    def rs(way, leg, c):
        return pltpu.make_async_remote_copy(
            src_ref=sbuf.at[way, lax.rem(leg, 2) * nc + c],
            dst_ref=rbuf.at[way, leg * nc + c],
            send_sem=rs_send.at[way, leg],
            recv_sem=rs_recv.at[way, jnp.where(leg == 0, 0, 1 + (leg - 1) * nc + c)],
            device_id={"tp": (right, left)[way]},
            device_id_type=pl.DeviceIdType.MESH,
        )

    def rs_all(way, leg):
        return pltpu.make_async_remote_copy(
            src_ref=sbuf.at[way, pl.ds(leg % 2 * nc, nc)],
            dst_ref=rbuf.at[way, pl.ds(leg * nc, nc)],
            send_sem=rs_send.at[way, leg],
            recv_sem=rs_recv.at[way, 0],
            device_id={"tp": (right, left)[way]},
            device_id_type=pl.DeviceIdType.MESH,
        )

    def attended(b):
        return q[pl.ds(pl.multiple_of(b * rows, rows), rows), :]

    def tiles(step, sides=(0, 1)):
        fetch(step + DEPTH - 1)
        for s in sides:
            wo_copy(step, s).wait()
        return lax.rem(step, DEPTH)

    def send_terms(leg, first, count=nc, ways=(0, 1), hold=False):
        aims = (jnp.where(leg == 0, right, opp), jnp.where(leg == 0, left, opp))
        sides = (1 - leg, leg)

        def body(t, _):
            step = first + t
            c = lax.rem(step, nc)
            slot = tiles(step, (0, 1) if len(ways) == 2 else (sides[ways[0]],))
            for way in ways:
                sbuf[way, leg * nc + c] = _dot(attended(aims[way]), wob[slot, sides[way]]).astype(bf16)
            if not hold:
                for way in ways:
                    rs(way, leg, c).start()

        lax.fori_loop(0, count, body, None)

    def send_held():
        def body(c, _):
            for way in range(2):

                @pl.when(jnp.logical_not(split) | ((way == 0) & (c < nc // 2)))
                def _(way=way):
                    rs(way, jnp.where(special, 1, 0), c).start()

        lax.fori_loop(0, nc, body, None)

    def leg2(c, _):
        slot = tiles((2 + more) * nc + c)
        terms = [_dot(attended(b), wob[slot, way]) for way, b in enumerate((right, left))]
        for way in range(2):
            rs(way, 1, c).wait_recv()
            sbuf[way, c] = (terms[way] + rbuf[way, nc + c].astype(f32)).astype(bf16)
        for way in range(2):
            rs(way, 2, c).start()

    def leg3(c, _):
        slot = tiles((3 + more) * nc + c)
        at = [pl.ds(pl.multiple_of(s * hw + c * CW, CW), CW) for s in range(2)]
        terms = [_dot(attended(me), wob[slot, s]) + y_ref[:, at[s]].astype(f32) for s in range(2)]
        for s in range(2):
            terms[s] += rbuf[1 - s, c].astype(f32)
        for s in range(2):
            rs(s, 2, c).wait_recv()
            y_ref[:, at[s]] = (terms[s] + rbuf[s, 2 * nc + c].astype(f32)).astype(bf16)

    with jax.named_scope("finish_early"):
        finishes(lambda b: jnp.where(special, b == opp, (b != me) & (b < opp)))

    @pl.when(special)
    def _():
        with jax.named_scope("wait_g2"):
            wait_ag(1, 0)
        with jax.named_scope("proj_g2"):
            project_kv(2, 0)
            project_q(2, 0)

    @pl.when((me == 1) | special)
    def _():
        with jax.named_scope("leg_early"):
            send_terms(jnp.where(special, 1, 0), 0, hold=True)

    @pl.when(split)
    def _():
        with jax.named_scope("leg_right"):
            send_terms(0, 0, nc // 2, (0,), hold=True)

    @pl.when(jnp.logical_not(special))
    def _():
        for part in range(2):
            with jax.named_scope("wait_g3"):
                wait_ag(2, part)
            if part == 1:
                send_held()
            with jax.named_scope("kv_g3"):
                project_kv(3, part)
            with jax.named_scope("pairs_sides"):

                def sides(t, _):
                    i = jnp.where(t == 0, right, left)

                    @pl.when(i > opp)
                    def _():
                        pair(i, opp, False, part)

                lax.fori_loop(0, 2, sides, None)

    @pl.when(special)
    def _():
        with jax.named_scope("wait_g2"):
            wait_ag(1, 1)
        send_held()
        with jax.named_scope("proj_g2"):
            project_kv(2, 1)
            project_q(2, 1)
        with jax.named_scope("pairs_sides"):
            pairs(lambda i, j: (i != me) & (i != opp))

    with jax.named_scope("finish_sides"):
        finishes(lambda b: (b != me) & (b != opp) & (special | (b > opp)))

    @pl.when(split)
    def _():
        with jax.named_scope("leg_left"):
            send_terms(0, nc // 2, nc, (1,))
            send_terms(0, nc // 2 * 3, nc // 2, (0,))

    @pl.when(jnp.logical_not(special))
    def _():
        with jax.named_scope("q_g3"):
            project_q(3)
        with jax.named_scope("pairs_opp"):
            pairs(lambda i, j: i == opp)
            finish(opp)

    with jax.named_scope("leg_second"):
        send_terms(jnp.where(special, 0, 1), (1 + more) * nc)
    with jax.named_scope("pairs_me"):
        pairs(lambda i, j: (i == me) & (j != me))

    for way in range(2):
        for leg in range(3):
            ag_all(way, leg).wait_send()
    with jax.named_scope("leg2"):
        finish(me)
        for way in range(2):
            rs_all(way, 0).wait_send()
        lax.fori_loop(0, nc, leg2, None)
    with jax.named_scope("leg3"):
        for way in range(2):
            rs_all(way, 0).wait_recv()
        lax.fori_loop(0, nc, leg3, None)
    with jax.named_scope("drain"):
        for way in range(2):
            for leg in (1, 2):
                rs_all(way, leg).wait_send()


def _table(tokens):
    half = HEAD // 2
    angle = np.arange(tokens, dtype=np.float64)[:, None] * float(THETA) ** (-np.arange(half, dtype=np.float64) / half)
    return np.concatenate([np.cos(angle), np.sin(angle)], -1).astype(np.float32)


def solution(mesh):
    n = mesh.shape["tp"]

    def step(x, gain, wq, wk, wv, wo):
        rows, width = x.shape
        tokens, qwidth = n * rows, wq.shape[1]
        heads = qwidth // HEAD
        nc = width // 2 // CW
        bf16, f32 = jnp.bfloat16, jnp.float32
        dma = pltpu.SemaphoreType.DMA
        hbm = pl.BlockSpec(memory_space=pl.ANY)
        return pl.pallas_call(
            functools.partial(_kernel, n),
            out_shape=pltpu.VMEM((rows, width), bf16),
            in_specs=[hbm] * 7,
            out_specs=pl.BlockSpec(memory_space=pltpu.VMEM),
            scratch_shapes=[
                pltpu.VMEM((width,), bf16),
                pltpu.VMEM((tokens, width), bf16),
                pltpu.VMEM((width, qwidth), bf16),
                pltpu.VMEM((width, 2 * HEAD), bf16),
                pltpu.VMEM((tokens, HEAD), f32),
                pltpu.VMEM((tokens, qwidth), bf16),
                pltpu.VMEM((tokens, HEAD), bf16),
                pltpu.VMEM((tokens, HEAD), bf16),
                pltpu.VMEM((n, heads, HEAD + EXTRA, rows), f32),
                pltpu.VMEM((n, heads, 8, rows), f32),
                pltpu.VMEM((DEPTH, 2, qwidth, CW), bf16),
                pltpu.VMEM((2, 2 * nc, rows, CW), bf16),
                pltpu.VMEM((2, 3 * nc, rows, CW), bf16),
                dma((4,)), dma, dma((qwidth // QT // 2,)), dma((3,)), dma((DEPTH, 2)),
                dma((2, 3)), dma((2, 5)), dma((2, 3)), dma((2, 1 + 2 * nc)),
            ],
            compiler_params=pltpu.CompilerParams(collective_id=0, has_side_effects=True, vmem_limit_bytes=VMEM),
        )(x, gain, wq, wk, wv, wo, _table(tokens))

    tokens, columns = P(("dp", "tp"), None), P(None, "tp")
    return jax.shard_map(
        step,
        mesh=mesh,
        in_specs=(tokens, P(None), columns, columns, columns, P("tp", None)),
        out_specs=tokens,
        check_vma=False,
    )
```

```python
import functools

import jax
import jax.numpy as jnp
import numpy as np
from jax import lax
from jax.experimental import pallas as pl
from jax.experimental.pallas import tpu as pltpu
from jax.sharding import PartitionSpec as P

HEAD = 128
THETA = 10000
NEG = -1e30
HIDDEN = 2 * NEG
LOG2E = 1.4426950408889634
SUB = 4
QT = 256
CW = 256
FINISH = 8
UNROLL = 8
DEPTH = 3
VMEM = 61 * 2**20 + 2**19
EXTRA = 16


def _dot(a, b, ca=1, cb=0):
    return lax.dot_general(a, b, (((ca,), (cb,)), ((), ())), preferred_element_type=jnp.float32)


def _kernel(n, x_ref, gain_ref, wq_ref, wk_ref, wv_ref, wo_ref, tab_ref, y_ref,
            gs, xg, wq, wkv, tab, q, k, v, mix, top, wob, sbuf, rbuf,
            x_sem, g_sem, wq_sem, w_sem, wo_sem, ag_send, ag_recv, rs_send, rs_recv):
    rows, width = x_ref.shape
    half = rows // 2
    sub = half // SUB
    qwidth = wq_ref.shape[1]
    heads = qwidth // HEAD
    hw = width // 2
    nc = hw // CW
    qn = qwidth // QT
    bf16, f32 = jnp.bfloat16, jnp.float32

    me = lax.axis_index("tp")
    right, left, opp = lax.rem(me + 1, n), lax.rem(me + n - 1, n), lax.rem(me + 2, n)

    X_CUTS = (0, 1, 2, 4, 2 * SUB)

    def x_copy(i):
        at = pl.ds(X_CUTS[i] * sub, (X_CUTS[i + 1] - X_CUTS[i]) * sub)
        return pltpu.make_async_copy(x_ref.at[at], y_ref.at[at], x_sem.at[i])

    def wq_copy(i):
        at = pl.ds(pl.multiple_of(i * 2 * QT, 2 * QT), 2 * QT)
        return pltpu.make_async_copy(wq_ref.at[:, at], wq.at[:, at], wq_sem.at[i])

    def wo_copy(step, s):
        c = lax.rem(step, nc)
        slot = lax.rem(step, DEPTH)
        return pltpu.make_async_copy(wo_ref.at[:, pl.ds(pl.multiple_of(s * hw + c * CW, CW), CW)], wob.at[slot, s], wo_sem.at[slot, s])

    split = (me == 0) | (me == 3)
    more = jnp.where(split, 1, 0)

    def fetch(step):
        for s in range(2):

            @pl.when((step < (4 + more) * nc) & jnp.logical_not(split & (step < 2 * nc) & ((step // (nc // 2) % 3 == 0) == (s == 0))))
            def _(s=s):
                wo_copy(step, s).start()

    g_copy = pltpu.make_async_copy(gain_ref, gs, g_sem)
    tab_copy = pltpu.make_async_copy(tab_ref, tab, w_sem.at[2])
    wk_copy = pltpu.make_async_copy(wk_ref, wkv.at[:, pl.ds(0, HEAD)], w_sem.at[0])
    wv_copy = pltpu.make_async_copy(wv_ref, wkv.at[:, pl.ds(HEAD, HEAD)], w_sem.at[1])

    barrier = pltpu.get_barrier_semaphore()
    for neighbour in (left, right):
        pl.semaphore_signal(barrier, inc=1, device_id={"tp": neighbour}, device_id_type=pl.DeviceIdType.MESH)
    g_copy.start()
    for i in range(len(X_CUTS) - 1):
        x_copy(i).start()

    def source(way, leg, i):
        if leg < 2:
            return (2 * i + (leg if way == 0 else 1 - leg)) * sub
        return rows + way * half + i * sub

    def target(way, leg, i):
        if leg == 0:
            return rows + way * half + i * sub
        if leg == 1:
            return 2 * rows + i // (SUB // 2) * half + way * (half // 2) + i % (SUB // 2) * sub
        return 3 * rows + (2 * i + way) * sub

    def arrival(leg, part):
        return 0 if leg == 0 else 2 * leg - 1 + part

    def part_of(leg, i):
        return i // (SUB // 2) if leg == 1 else i // (SUB - 1)

    def ag(way, leg, i):
        return pltpu.make_async_remote_copy(
            src_ref=xg.at[pl.ds(source(way, leg, i), sub)],
            dst_ref=xg.at[pl.ds(target(way, leg, i), sub)],
            send_sem=ag_send.at[way, leg],
            recv_sem=ag_recv.at[way, arrival(leg, part_of(leg, i))],
            device_id={"tp": (right, left)[way]},
            device_id_type=pl.DeviceIdType.MESH,
        )

    def ag_all(way, leg, part=None):
        pieces = SUB if part is None else sum(part_of(leg, i) == part for i in range(SUB))
        at = pl.ds((min(leg, 1) * 2 + way) * half, pieces * sub)
        return pltpu.make_async_remote_copy(
            src_ref=xg.at[at],
            dst_ref=xg.at[at],
            send_sem=ag_send.at[way, leg],
            recv_sem=ag_recv.at[way, arrival(leg, part or 0)],
            device_id={"tp": (right, left)[way]},
            device_id_type=pl.DeviceIdType.MESH,
        )

    step16 = 16

    def norm(start, count):
        def body(t, _):
            at = pl.ds(pl.multiple_of(start + t * step16, step16), step16)
            wide = y_ref[at, :].astype(f32)
            scale = lax.rsqrt(jnp.mean(wide * wide, -1, keepdims=True) + 1e-6)
            xg[at, :] = (wide * scale * gs[...].astype(f32)[None, :]).astype(bf16)

        lax.fori_loop(0, count // step16, body, None)

    with jax.named_scope("norm"):
        g_copy.wait()
        for i in range(SUB):
            for p in range(2):
                if 2 * i + p in X_CUTS:
                    x_copy(X_CUTS.index(2 * i + p)).wait()
                if 2 * i + p == X_CUTS[-2]:
                    wk_copy.start()
                    wv_copy.start()
                    tab_copy.start()
                    for j in range(qn // 2):
                        wq_copy(j).start()
                norm((2 * i + p) * sub, sub)
                if i == 0 and p == 0:
                    pl.semaphore_wait(barrier, 2)
                ag(p, 0, i).start()
        for way, late in ((0, 1), (1, 3)):

            @pl.when(me != late)
            def _(way=way):
                for i in range(SUB):
                    ag(way, 1, i).start()

        for ahead in range(DEPTH - 1):
            fetch(ahead)

    lane = lax.broadcasted_iota(jnp.int32, (1, HEAD), 1)
    low = lane < HEAD // 2

    def turn(t, at):
        cs = tab[pl.ds(pl.multiple_of(at, sub), t.shape[0]), :]
        sc = pltpu.roll(cs, HEAD // 2, 1)
        t = t.astype(f32)
        return (t * jnp.where(low, cs, sc) + pltpu.roll(t, HEAD // 2, 1) * jnp.where(low, -sc, cs)).astype(bf16)

    def runs(g):
        if g in (0, 3):
            return ((0, rows, (me if g == 0 else opp) * rows),)
        if g == 1:
            return tuple((p * half + i * sub, sub, b * rows + (2 * i + p) * sub) for p, b in enumerate((left, right)) for i in range(SUB))
        return tuple((target(p, 1, i) - 2 * rows, sub, b * rows + (2 * i + 1 - p) * sub) for i in range(SUB) for p, b in enumerate((left, right)))

    LAST = ((0, rows - 2 * sub), (rows - 2 * sub, 2 * sub))

    def rows_of(g, part):
        if part is None:
            return 0, rows, runs(g)
        if g == 3:
            first, count = LAST[part]
            return first, count, ((0, count, runs(3)[0][2] + first),)
        first = part * half
        return first, half, tuple((row - first, size, at) for row, size, at in runs(g) if first <= row < first + half)

    def project_kv(g, part=None):
        first, count, pieces = rows_of(g, part)
        t = _dot(xg[pl.ds(g * rows + first, count), :], wkv[...]).astype(bf16)
        for row, size, at in pieces:
            at = pl.multiple_of(at, sub)
            k[pl.ds(at, size), :] = turn(t[row : row + size, :HEAD], at)
            v[pl.ds(at, size), :] = t[row : row + size, HEAD:]

    def project_q(g, part=None):
        first, count, pieces = rows_of(g, part)

        def body(j, _):
            if g == 0:

                @pl.when(lax.rem(j, 2) == 0)
                def _():
                    wq_copy(j // 2).wait()

            t = _dot(xg[pl.ds(g * rows + first, count), :], wq[:, pl.ds(pl.multiple_of(j * QT, QT), QT)]).astype(bf16)
            for row, size, at in pieces:
                at = pl.multiple_of(at, sub)
                for e in range(QT // HEAD):
                    part_ = t[row : row + size, e * HEAD : (e + 1) * HEAD]
                    q[pl.ds(at, size), pl.ds(pl.multiple_of(j * QT + e * HEAD, HEAD), HEAD)] = turn(part_, at)

        lax.fori_loop(0, qn, body, None)

    e2 = HEAD**-0.5 * LOG2E

    def pair(i, j, masked, part=None):
        first, count = (0, rows) if part is None else LAST[part]
        keys = pl.ds(pl.multiple_of(j * rows + first, 2 * sub), count)
        kj = k[keys, :]
        vj = jnp.concatenate([v[keys, :].astype(f32).T.astype(bf16), jnp.ones((EXTRA, count), bf16)], axis=0)
        if masked:
            ok = lax.broadcasted_iota(jnp.int32, (rows, rows), 0) <= lax.broadcasted_iota(jnp.int32, (rows, rows), 1)

        unroll = UNROLL if count > half else 2 * UNROLL

        def body(m, _):
            hs = [m * unroll + u for u in range(unroll)]
            scores = [_dot(kj, q[pl.ds(pl.multiple_of(i * rows, rows), rows), pl.ds(pl.multiple_of(h * HEAD, HEAD), HEAD)], 1, 1) for h in hs]
            weights, keeps = [], []
            for h, s in zip(hs, scores):
                if masked:
                    s = jnp.where(ok, s, HIDDEN)
                old = top[i, h, 0:1, :]
                new = jnp.maximum(old, s.max(axis=0, keepdims=True))
                top[i, h, 0:1, :] = new
                weights.append(jnp.exp2((s - new) * e2).astype(bf16))
                keeps.append(jnp.exp2((old - new) * e2))
            for h, p, keep in zip(hs, weights, keeps):
                mix[i, h] = mix[i, h] * keep + _dot(vj, p)

        lax.fori_loop(0, heads // unroll, body, None)

    def pairs(wanted):
        def body(t, _):
            i, j = t // n, lax.rem(t, n)

            @pl.when((i > j) & wanted(i, j))
            def _():
                pair(i, j, False)

            @pl.when((i == j) & wanted(i, j))
            def _():
                pair(i, j, True)

        lax.fori_loop(0, n * n, body, None)

    def finish(i):
        def body(m, _):
            for u in range(FINISH):
                h = m * FINISH + u
                out = mix[i, h, :HEAD, :] * (1 / mix[i, h, HEAD : HEAD + 1, :])
                q[pl.ds(pl.multiple_of(i * rows, rows), rows), pl.ds(pl.multiple_of(h * HEAD, HEAD), HEAD)] = out.T.astype(bf16)

        lax.fori_loop(0, heads // FINISH, body, None)

    with jax.named_scope("own_proj"):
        tab_copy.wait()
        wk_copy.wait()
        wv_copy.wait()
        project_kv(0)
        project_q(0)

    def clear(t, _):
        i, h = t // heads, lax.rem(t, heads)
        mix[i, h] = jnp.zeros((HEAD + EXTRA, rows), f32)
        top[i, h] = jnp.full((8, rows), NEG, f32)

    with jax.named_scope("own_pair"):
        lax.fori_loop(0, n * heads, clear, None)
        pair(me, me, True)

    special = opp == 0

    def known(b):
        return (b == me) | ((b == opp) == special)

    def wait_ag(leg, *parts):
        for part in parts or (None,):
            for way in range(2):
                ag_all(way, leg, part).wait_recv()

    with jax.named_scope("wait_g1"):
        wait_ag(0)
        for i in range(SUB):
            for way in range(2):
                ag(way, 2, i).start()
        for way, late in ((0, 1), (1, 3)):

            @pl.when(me == late)
            def _(way=way):
                for i in range(SUB):
                    ag(way, 1, i).start()

    with jax.named_scope("proj_g1"):
        project_kv(1)
        project_q(1)

    @pl.when(jnp.logical_not(special))
    def _():
        for part in range(2):
            with jax.named_scope("wait_g2"):
                wait_ag(1, part)
            with jax.named_scope("proj_g2"):
                project_kv(2, part)
                project_q(2, part)

    @pl.when(special)
    def _():
        for part in range(2):
            with jax.named_scope("wait_g3"):
                wait_ag(2, part)
            with jax.named_scope("proj_g3"):
                project_kv(3, part)
                project_q(3, part)

    with jax.named_scope("pairs_early"):
        pairs(lambda i, j: known(i) & known(j) & (i != me))

    def finishes(wanted):
        def body(b, _):
            @pl.when(wanted(b))
            def _():
                finish(b)

        lax.fori_loop(0, n, body, None)

    def rs(way, leg, c):
        return pltpu.make_async_remote_copy(
            src_ref=sbuf.at[way, lax.rem(leg, 2) * nc + c],
            dst_ref=rbuf.at[way, leg * nc + c],
            send_sem=rs_send.at[way, leg],
            recv_sem=rs_recv.at[way, jnp.where(leg == 0, 0, jnp.where(leg == 1, 1 + c // 2, 1 + nc // 2 + c))],
            device_id={"tp": (right, left)[way]},
            device_id_type=pl.DeviceIdType.MESH,
        )

    def rs_all(way, leg):
        return pltpu.make_async_remote_copy(
            src_ref=sbuf.at[way, pl.ds(leg % 2 * nc, nc)],
            dst_ref=rbuf.at[way, pl.ds(leg * nc, nc)],
            send_sem=rs_send.at[way, leg],
            recv_sem=rs_recv.at[way, 0],
            device_id={"tp": (right, left)[way]},
            device_id_type=pl.DeviceIdType.MESH,
        )

    def attended(b):
        return q[pl.ds(pl.multiple_of(b * rows, rows), rows), :]

    def tiles(step, sides=(0, 1)):
        fetch(step + DEPTH - 1)
        for s in sides:
            wo_copy(step, s).wait()
        return lax.rem(step, DEPTH)

    def send_terms(leg, first, count=nc, ways=(0, 1), hold=False):
        aims = (jnp.where(leg == 0, right, opp), jnp.where(leg == 0, left, opp))
        sides = (1 - leg, leg)

        def body(t, _):
            step = first + t
            c = lax.rem(step, nc)
            slot = tiles(step, (0, 1) if len(ways) == 2 else (sides[ways[0]],))
            for way in ways:
                sbuf[way, leg * nc + c] = _dot(attended(aims[way]), wob[slot, sides[way]]).astype(bf16)
            if not hold:
                for way in ways:
                    rs(way, leg, c).start()

        lax.fori_loop(0, count, body, None)

    def send_held():
        def body(c, _):
            for way in range(2):

                @pl.when(jnp.logical_not(split) | ((way == 0) & (c < nc // 2)))
                def _(way=way):
                    rs(way, 0, c).start()

        lax.fori_loop(0, nc, body, None)

    def rs_two(way, c):
        return pltpu.make_async_remote_copy(
            src_ref=sbuf.at[way, pl.ds(nc + c, 2)],
            dst_ref=rbuf.at[way, pl.ds(nc + c, 2)],
            send_sem=rs_send.at[way, 1],
            recv_sem=rs_recv.at[way, 1 + c // 2],
            device_id={"tp": (right, left)[way]},
            device_id_type=pl.DeviceIdType.MESH,
        )

    def leg2(c, _):
        slot = tiles((2 + more) * nc + c)
        terms = [_dot(attended(b), wob[slot, way]) for way, b in enumerate((right, left))]

        @pl.when(lax.rem(c, 2) == 0)
        def _():
            for way in range(2):
                rs_two(way, c).wait_recv()

        for way in range(2):
            sbuf[way, c] = (terms[way] + rbuf[way, nc + c].astype(f32)).astype(bf16)
        for way in range(2):
            rs(way, 2, c).start()

    def leg3(c, _):
        slot = tiles((3 + more) * nc + c)
        at = [pl.ds(pl.multiple_of(s * hw + c * CW, CW), CW) for s in range(2)]
        terms = [_dot(attended(me), wob[slot, s]) + y_ref[:, at[s]].astype(f32) for s in range(2)]
        for s in range(2):
            terms[s] += rbuf[1 - s, c].astype(f32)
        for s in range(2):
            rs(s, 2, c).wait_recv()
            y_ref[:, at[s]] = (terms[s] + rbuf[s, 2 * nc + c].astype(f32)).astype(bf16)

    with jax.named_scope("finish_early"):
        finishes(lambda b: jnp.where(special, b == opp, (b != me) & (b < opp)))

    @pl.when(special)
    def _():
        with jax.named_scope("leg_early"):
            send_terms(1, 0)
        with jax.named_scope("wait_g2"):
            wait_ag(1, 0)
        with jax.named_scope("proj_g2"):
            project_kv(2, 0)
            project_q(2, 0)

    @pl.when(me == 1)
    def _():
        with jax.named_scope("leg_early"):
            send_terms(0, 0, hold=True)

    @pl.when(split)
    def _():
        with jax.named_scope("leg_right"):
            send_terms(0, 0, nc // 2, (0,), hold=True)

    @pl.when(jnp.logical_not(special))
    def _():
        for part in range(2):
            with jax.named_scope("wait_g3"):
                wait_ag(2, part)
            if part == 1:
                send_held()
            with jax.named_scope("kv_g3"):
                project_kv(3, part)
            with jax.named_scope("pairs_sides"):

                def sides(t, _):
                    i = jnp.where(t == 0, right, left)

                    @pl.when(i > opp)
                    def _():
                        pair(i, opp, False, part)

                lax.fori_loop(0, 2, sides, None)

    @pl.when(special)
    def _():
        with jax.named_scope("wait_g2"):
            wait_ag(1, 1)
        with jax.named_scope("proj_g2"):
            project_kv(2, 1)
            project_q(2, 1)
        with jax.named_scope("pairs_sides"):
            pairs(lambda i, j: (i != me) & (i != opp))

    with jax.named_scope("finish_sides"):
        finishes(lambda b: (b != me) & (b != opp) & (special | (b > opp)))

    @pl.when(split)
    def _():
        with jax.named_scope("leg_left"):
            send_terms(0, nc // 2, nc, (1,))
            send_terms(0, nc // 2 * 3, nc // 2, (0,))

    @pl.when(jnp.logical_not(special))
    def _():
        with jax.named_scope("q_g3"):
            project_q(3)
        with jax.named_scope("pairs_opp"):
            pairs(lambda i, j: i == opp)
            finish(opp)

    with jax.named_scope("leg_second"):
        send_terms(jnp.where(special, 0, 1), (1 + more) * nc)
    with jax.named_scope("pairs_me"):
        pairs(lambda i, j: (i == me) & (j != me))

    for way in range(2):
        for leg in range(3):
            ag_all(way, leg).wait_send()
    with jax.named_scope("leg2"):
        finish(me)
        for way in range(2):
            rs_all(way, 0).wait_send()
        lax.fori_loop(0, nc, leg2, None)
    with jax.named_scope("leg3"):
        for way in range(2):
            rs_all(way, 0).wait_recv()
        lax.fori_loop(0, nc, leg3, None)
    with jax.named_scope("drain"):
        for way in range(2):
            for leg in (1, 2):
                rs_all(way, leg).wait_send()


def _table(tokens):
    half = HEAD // 2
    angle = np.arange(tokens, dtype=np.float64)[:, None] * float(THETA) ** (-np.arange(half, dtype=np.float64) / half)
    return np.concatenate([np.cos(angle), np.sin(angle)], -1).astype(np.float32)


def solution(mesh):
    n = mesh.shape["tp"]

    def step(x, gain, wq, wk, wv, wo):
        rows, width = x.shape
        tokens, qwidth = n * rows, wq.shape[1]
        heads = qwidth // HEAD
        nc = width // 2 // CW
        bf16, f32 = jnp.bfloat16, jnp.float32
        dma = pltpu.SemaphoreType.DMA
        hbm = pl.BlockSpec(memory_space=pl.ANY)
        return pl.pallas_call(
            functools.partial(_kernel, n),
            out_shape=pltpu.VMEM((rows, width), bf16),
            in_specs=[hbm] * 7,
            out_specs=pl.BlockSpec(memory_space=pltpu.VMEM),
            scratch_shapes=[
                pltpu.VMEM((width,), bf16),
                pltpu.VMEM((tokens, width), bf16),
                pltpu.VMEM((width, qwidth), bf16),
                pltpu.VMEM((width, 2 * HEAD), bf16),
                pltpu.VMEM((tokens, HEAD), f32),
                pltpu.VMEM((tokens, qwidth), bf16),
                pltpu.VMEM((tokens, HEAD), bf16),
                pltpu.VMEM((tokens, HEAD), bf16),
                pltpu.VMEM((n, heads, HEAD + EXTRA, rows), f32),
                pltpu.VMEM((n, heads, 8, rows), f32),
                pltpu.VMEM((DEPTH, 2, qwidth, CW), bf16),
                pltpu.VMEM((2, 2 * nc, rows, CW), bf16),
                pltpu.VMEM((2, 3 * nc, rows, CW), bf16),
                dma((4,)), dma, dma((qwidth // QT // 2,)), dma((3,)), dma((DEPTH, 2)),
                dma((2, 3)), dma((2, 5)), dma((2, 3)), dma((2, 1 + nc // 2 + nc)),
            ],
            compiler_params=pltpu.CompilerParams(collective_id=0, has_side_effects=True, vmem_limit_bytes=VMEM),
        )(x, gain, wq, wk, wv, wo, _table(tokens))

    tokens, columns = P(("dp", "tp"), None), P(None, "tp")
    return jax.shard_map(
        step,
        mesh=mesh,
        in_specs=(tokens, P(None), columns, columns, columns, P("tp", None)),
        out_specs=tokens,
        check_vma=False,
    )
```
